256 devices in a mesh: ctx: 64 (over z, y, core), head: 4 (over x).
Axes of the slice: x: 4, y: 4, z: 8, core: 2. Of those that a mesh axis runs over, the one named last changes fastest.
Arguments:
- query_latent: bfloat16 [128, 128, 576], P(None, 'head'), may hold values from -7 to 7
- key_latent: bfloat16 [131072, 576], P('ctx'), may hold values from -6 to 6
- index_query: bfloat16 [128, 64, 128], P(None, 'head'), may hold values from -0.5 to 0.5
- index_weight: bfloat16 [128, 64], P(None, 'head'), may hold values from -110 to 110
- index_key: bfloat16 [131072, 128], P('ctx'), may hold values from -6 to 6
- positions: int32 [128], replicated, may hold values from 32768 to 131071
Outputs:
- target: float32 [128, 131072], P('head', 'ctx')
- divergence: float32 [128], P('head')
The draws below stay inside these ranges and needn't reach their ends.
Inputs may be any that keep to these rules, and one draw needn't show every extreme that they name: Row q may attend to keys 0 through positions[q].
All inputs are finite; a program needn't handle non-finite values.
Results may differ from the reference program's by a relative error of at most 0.0003.
Values may be sent and summed in bfloat16 or wider, within the bound.
A program may use at most 128 MiB of HBM per device.

```python
import jax
import jax.numpy as jnp
from jax import lax

H = 128
QK = 576
IH = 64
ID = 128
Q = 128
KEYS = 131072


def key_values(key):
    return jnp.clip(jax.random.normal(jax.random.fold_in(key, 11), (KEYS, QK), jnp.float32), -6.0, 6.0)


def draw_key_latent(key, part):
    return key_values(key).astype(jnp.bfloat16)


def draw_query_latent(key, part):
    result = jnp.clip(jax.random.normal(jax.random.fold_in(key, 12), (Q, H, QK), jnp.float32), -6.0, 6.0) / 24.0
    return result.astype(jnp.bfloat16)


def draw_index_weight(key, part):
    result = jnp.clip(jax.random.normal(jax.random.fold_in(key, 21), (Q, IH), jnp.float32), -6.0, 6.0)
    return result.astype(jnp.bfloat16)


def set_ends(entries, key, smallest, largest):
    longest = entries.shape.index(max(entries.shape))
    spots = []
    for shift in (0, 1):
        where = [jax.random.randint(jax.random.fold_in(key, axis), (), 0, length) for axis, length in enumerate(entries.shape)]
        where[longest] = (where[longest] + shift) % entries.shape[longest]
        spots.append(tuple(where))
    return entries.at[spots[0]].set(smallest).at[spots[1]].set(largest)


def levels(stream_key, extent, split, low, high):
    gain, own = 1.0, jax.random.fold_in(stream_key, 6)
    for position, parts in split:
        steps = jnp.exp(jax.random.uniform(jax.random.fold_in(own, position), (parts,), jnp.float32, low / len(split), high / len(split)))
        gain = gain * jnp.repeat(steps, extent[position] // parts).reshape([-1 if axis == position else 1 for axis in range(len(extent))])
    return gain


def bell_draw(own_key, shape, scale, limit, pieces=(), kind=jnp.bfloat16):
    factor_of = levels(own_key, shape, pieces, -0.22, 0.18) if pieces else 1.0
    entries = jax.random.normal(own_key, shape, jnp.float32) * scale * factor_of
    return jnp.minimum(jnp.maximum(entries, -limit), limit).astype(kind)


def setup_inputs(seed: int = 0) -> dict:
    arg_keys = jax.random.split(jax.random.key(seed), 7)
    query_latent = draw_query_latent(jax.random.fold_in(arg_keys[6], 71), 0)
    key_latent = draw_key_latent(jax.random.fold_in(arg_keys[6], 71), 0)
    index_query = bell_draw(arg_keys[2], (Q, IH, ID), ID ** -0.5, 0.5, ((1, 4),))
    index_weight = draw_index_weight(jax.random.fold_in(arg_keys[6], 71), 0)
    index_key = bell_draw(arg_keys[4], (KEYS, ID), 1.0, 6.0, ((0, 64),))
    positions = set_ends(jax.random.randint(arg_keys[5], (Q,), KEYS // 4, KEYS), jax.random.fold_in(arg_keys[5], 1), KEYS // 4, KEYS - 1).astype(jnp.int32)
    return {"query_latent": query_latent, "key_latent": key_latent, "index_query": index_query, "index_weight": index_weight, "index_key": index_key, "positions": positions}


def reference(query_latent, key_latent, index_query, index_weight, index_key, positions):
    key_float = key_latent.astype(jnp.float32)
    allowed = jnp.arange(KEYS, dtype=jnp.int32)[None, :] <= positions[:, None]

    def head_step(accum, query_head):
        scores = jnp.dot(query_head.astype(jnp.float32), key_float.T, precision=lax.Precision.HIGHEST)
        highest = jnp.max(jnp.where(allowed, scores, -1e30), axis=1, keepdims=True)
        weights = jnp.where(allowed, jnp.exp(scores - highest), 0.0)
        return accum + weights / jnp.sum(weights, axis=1, keepdims=True), None

    start = jnp.zeros((Q, KEYS), jnp.float32)
    summed, _ = lax.scan(head_step, start, jnp.moveaxis(query_latent, 1, 0))
    target = summed / H

    index_float = index_key.astype(jnp.float32)

    def index_step(accum, pair):
        query_head, weight_col = pair
        raw = jnp.dot(query_head.astype(jnp.float32), index_float.T, precision=lax.Precision.HIGHEST)
        return accum + weight_col.astype(jnp.float32)[:, None] * jnp.maximum(raw, 0.0), None

    logits, _ = lax.scan(index_step, start, (jnp.moveaxis(index_query, 1, 0), index_weight.T))
    peak = jnp.max(jnp.where(allowed, logits, -1e30), axis=1)
    denom = jnp.sum(jnp.where(allowed, jnp.exp(logits - peak[:, None]), 0.0), axis=1)
    spread = peak + jnp.log(denom)
    positive = target > 0
    entropy_terms = jnp.where(positive, target * jnp.log(jnp.where(positive, target, 1.0)), 0.0)
    cross = jnp.sum(jnp.where(allowed, entropy_terms - target * logits, 0.0), axis=1)
    divergence = cross + spread * jnp.sum(target, axis=1)
    return target, divergence
```

```python
import jax
import jax.numpy as jnp
from jax import lax
from jax.experimental import pallas as pl
from jax.experimental.pallas import tpu as pltpu
from jax.sharding import Mesh
from jax.sharding import PartitionSpec as P

H = 128
CTX = ("z", "y", "c")
NEG = -1e30
MESH = pl.DeviceIdType.MESH
f32 = jnp.float32
KL = 2048
NE = 6


def lane_swap(a, b, keep, shift):
    return (
        jnp.where(keep, a, pltpu.roll(b, shift, 1)),
        jnp.where(keep, pltpu.roll(a, 128 - shift, 1), b),
    )


def lane_groups(shape):
    lane = lax.broadcasted_iota(jnp.int32, shape, 1)
    return (lane // 8) % 2 == 0, (lane // 16) % 2 == 0


def build_weights(q_ref, w_ref, i):
    even, low = lane_groups((576, 128))
    a = [q_ref[4 * i + g] for g in range(4)]
    a[0], a[1] = lane_swap(a[0], a[1], even, 8)
    a[2], a[3] = lane_swap(a[2], a[3], even, 8)
    a[0], a[2] = lane_swap(a[0], a[2], low, 16)
    a[1], a[3] = lane_swap(a[1], a[3], low, 16)
    for c in range(4):
        w_ref[c, :, pl.ds(pl.multiple_of(i * 128, 128), 128)] = a[c]


def dot_into(s_ref, k_ref, w_ref, t):
    w = w_ref[t // 4, :, pl.ds(pl.multiple_of((t % 4) * 256, 256), 256)]
    s_ref[...] = lax.dot_general(
        k_ref[...], w, (((1,), (0,)), ((), ())), preferred_element_type=f32
    )


def exp_from(s_ref, e_ref, top_ref, sum_ref, thr_ref, t):
    th = thr_ref[t // 4]
    acc = [[None] * 4 for _ in range(2)]
    for k in range(KL // 8):
        m = th >= 8 * k
        for j in range(2):
            v = jnp.where(m, s_ref[8 * k : 8 * k + 8, j * 128 : (j + 1) * 128], NEG)
            a = k % 4
            acc[j][a] = v if acc[j][a] is None else jnp.maximum(acc[j][a], v)
    tops = []
    for j in range(2):
        m = jnp.maximum(
            jnp.maximum(acc[j][0], acc[j][1]), jnp.maximum(acc[j][2], acc[j][3])
        )
        m = jnp.max(m, axis=0, keepdims=True)
        top_ref[pl.ds(2 * t + j, 1), :] = m
        tops.append(jnp.broadcast_to(m, (8, 128)))
    acc = [[None] * 4 for _ in range(2)]
    for k in range(KL // 8):
        m = th >= 8 * k
        for j in range(2):
            s = s_ref[8 * k : 8 * k + 8, j * 128 : (j + 1) * 128]
            v = jnp.where(m, jnp.exp(s - tops[j]), 0.0)
            e_ref[2 * t + j, 8 * k : 8 * k + 8, :] = v
            a = k % 4
            acc[j][a] = v if acc[j][a] is None else acc[j][a] + v
    for j in range(2):
        m = (acc[j][0] + acc[j][1]) + (acc[j][2] + acc[j][3])
        sum_ref[pl.ds(2 * t + j, 1), :] = jnp.sum(m, axis=0, keepdims=True)


def lse_of(top, total):
    some = total > 0
    return jnp.where(some, top + jnp.log(jnp.where(some, total, 1.0)), NEG)


def merge_lse(v):
    m = jnp.max(v, axis=0)
    return m + jnp.log(jnp.sum(jnp.exp(v - m[None]), axis=0))


def as_row(column):
    n = column.shape[0]
    row = lax.broadcasted_iota(jnp.int32, (n, 128), 0)
    lane = lax.broadcasted_iota(jnp.int32, (n, 128), 1)
    return jnp.sum(jnp.where(row == lane, column, 0.0), axis=0, keepdims=True)


def kernel(
    pos_s, pos_v, q_hbm, k_hbm, iq_hbm, iw_hbm, ik_hbm,
    tgt_ref, div_ref,
    q_ref, kt_ref, k_ref, w_ref, s0_ref, s1_ref, e_ref, top_ref, sum_ref, thr_ref,
    iq_ref, iw_ref, ik_ref, wc_ref, lg_ref, u_ref, part_ref, got_ref,
    ab_ref, bb_ref, l_ref, pc_ref, cm_ref,
    in_sem, ix_sem, ix_send, ix_recv, a_send, a_recv, b_send, b_recv, r_send, r_recv,
):
    z, y, c0, x = (lax.axis_index(n) for n in ("z", "y", "c", "x"))
    me_a = y * 2 + c0
    base = ((z * 4 + y) * 2 + c0) * KL

    def x_peer(d):
        return {"z": z, "y": y, "c": c0, "x": lax.rem(x + d, 4)}

    def a_peer(d):
        p = lax.rem(me_a + d, 8)
        return {"z": z, "y": p // 2, "c": lax.rem(p, 2), "x": x}

    def b_peer(d):
        return {"z": lax.rem(z + d, 8), "y": y, "c": c0, "x": x}

    copies = [
        pltpu.make_async_copy(k_hbm, kt_ref, in_sem.at[0]),
        pltpu.make_async_copy(q_hbm.at[pl.ds(0, 16)], q_ref.at[pl.ds(0, 16)], in_sem.at[1]),
        pltpu.make_async_copy(q_hbm.at[pl.ds(16, 16)], q_ref.at[pl.ds(16, 16)], in_sem.at[2]),
        pltpu.make_async_copy(ik_hbm, ik_ref, in_sem.at[3]),
    ]
    for cp in copies:
        cp.start()
    own_iq = pltpu.make_async_copy(
        iq_hbm.at[pl.ds(pl.multiple_of(x * 32, 32), 32)], iq_ref.at[x], ix_sem.at[0]
    )
    own_iw = pltpu.make_async_copy(iw_hbm, iw_ref.at[x], ix_sem.at[1])
    own_iq.start()
    own_iw.start()

    barrier = pltpu.get_barrier_semaphore()
    for d in range(1, 4):
        pl.semaphore_signal(barrier, inc=1, device_id=x_peer(d), device_id_type=MESH)
    for d in range(1, 8):
        pl.semaphore_signal(barrier, inc=1, device_id=a_peer(d), device_id_type=MESH)
        pl.semaphore_signal(barrier, inc=1, device_id=b_peer(d), device_id_type=MESH)

    group = (lax.broadcasted_iota(jnp.int32, (8, 128), 1) // 8) % 4
    sub = lax.broadcasted_iota(jnp.int32, (8, 128), 0)
    pos8 = jnp.broadcast_to(pos_v[...], (8, 128))
    for c in range(4):
        th = pos8
        for g in range(4):
            if g != c:
                th = jnp.where(group == g, pltpu.roll(pos8, (8 * (g - c)) % 128, 1), th)
        thr_ref[c] = th - base - sub
    for q in range(32):
        pc_ref[q : q + 1, :] = jnp.full((1, 128), pos_s[x * 32 + q] - base, jnp.int32)

    copies[0].wait()
    for n in range(KL // 128):
        k_ref[n * 128 : (n + 1) * 128, :] = kt_ref[:, n * 128 : (n + 1) * 128].T
    copies[1].wait()
    copies[2].wait()

    @pl.loop(0, 8)
    def _(i):
        build_weights(q_ref, w_ref, i)

    dot_into(s0_ref, k_ref, w_ref, 0)

    pl.semaphore_wait(barrier, 17)
    own_iq.wait()
    own_iw.wait()

    def ix_copies(d):
        peer = x_peer(d)
        to = lax.rem(x + d, 4)
        return [
            pltpu.make_async_remote_copy(
                iq_hbm.at[pl.ds(pl.multiple_of(to * 32, 32), 32)], iq_ref.at[x],
                ix_send.at[0], ix_recv.at[0], device_id=peer, device_id_type=MESH,
            ),
            pltpu.make_async_remote_copy(
                iw_hbm, iw_ref.at[x],
                ix_send.at[1], ix_recv.at[1], device_id=peer, device_id_type=MESH,
            ),
        ]

    for d in range(1, 4):
        for cp in ix_copies(d):
            cp.start()

    def exchange_start(buf, me, e, value, send, recv, peer):
        buf[e, me] = value
        for d in range(1, 8):
            pltpu.make_async_remote_copy(
                buf.at[e, me], buf.at[e, me], send.at[e], recv.at[e],
                device_id=peer(d), device_id_type=MESH,
            ).start()

    def seven(buf, e, send, recv):
        return pltpu.make_async_remote_copy(
            buf.at[e, pl.ds(0, 7)], buf.at[e, pl.ds(0, 7)], send.at[e], recv.at[e],
            device_id=x_peer(1), device_id_type=MESH,
        )

    def a_start(e, value):
        exchange_start(ab_ref, me_a, e, value, a_send, a_recv, a_peer)

    def a_done(e):
        seven(ab_ref, e, a_send, a_recv).wait_recv()
        return ab_ref[e]

    def b_start(e, value):
        exchange_start(bb_ref, z, e, value, b_send, b_recv, b_peer)

    def b_done(e):
        seven(bb_ref, e, b_send, b_recv).wait_recv()
        return bb_ref[e]

    def stats_out(c):
        rows = pl.ds(pl.multiple_of(c * 8, 8), 8)
        a_start(c, lse_of(top_ref[rows, :], sum_ref[rows, :]))

    def middle(c):
        b_start(c, merge_lse(a_done(c)))

    def head_sum(c):
        lse = merge_lse(b_done(c))
        rows = pl.ds(pl.multiple_of(c * 8, 8), 8)
        l_ref[...] = jnp.exp(top_ref[rows, :] - lse) * (1.0 / H)
        coef = [jnp.broadcast_to(l_ref[i : i + 1, :], (8, 128)) for i in range(8)]
        even, low = lane_groups((8, 128))

        def pair(a, b, keep, shift):
            other = jnp.where(keep, b, a)
            return jnp.where(keep, a, b) + jnp.where(
                keep, pltpu.roll(other, 128 - shift, 1), pltpu.roll(other, shift, 1)
            )

        @pl.loop(0, 8)
        def _(kb):
            for k in range(8):
                acc = []
                for g in range(4):
                    at = pl.ds(pl.multiple_of(g * 512 + kb * 64, 64) + k * 8, 8)
                    s = e_ref[c * 8, at, :] * coef[0]
                    for i in range(1, 8):
                        s = s + e_ref[c * 8 + i, at, :] * coef[i]
                    acc.append(s)
                u_ref[pl.ds(pl.multiple_of(kb * 64, 64) + k * 8, 8), :] = pair(
                    pair(acc[0], acc[1], even, 8), pair(acc[2], acc[3], even, 8), low, 16
                )

        for n in range(4):
            part_ref[c, :, n * 128 : (n + 1) * 128] = u_ref[n * 128 : (n + 1) * 128, :].T
        for d in range(1, 4):
            to = lax.rem(x + d, 4)
            pltpu.make_async_remote_copy(
                part_ref.at[c, pl.ds(pl.multiple_of(to * 32, 32), 32)], got_ref.at[c, x],
                r_send.at[c], r_recv.at[c], device_id=x_peer(d), device_id_type=MESH,
            ).start()

    def three(c):
        return pltpu.make_async_remote_copy(
            got_ref.at[c, pl.ds(0, 3)], got_ref.at[c, pl.ds(0, 3)],
            r_send.at[c], r_recv.at[c], device_id=x_peer(1), device_id_type=MESH,
        )

    def own_rows(c):
        three(c).wait_recv()
        got_ref[c, x] = part_ref[c, pl.ds(pl.multiple_of(x * 32, 32), 32)]
        cross = mass = None
        for g in range(4):
            t = got_ref[c, 0, 8 * g : 8 * g + 8]
            for k in range(1, 4):
                t = t + got_ref[c, k, 8 * g : 8 * g + 8]
            lg = lg_ref[8 * c : 8 * c + 8, g * 512 : (g + 1) * 512]
            tgt_ref[8 * c : 8 * c + 8, g * 512 : (g + 1) * 512] = t
            positive = t > 0
            term = jnp.where(positive, t * jnp.log(jnp.where(positive, t, 1.0)), 0.0) - t * lg
            cross = term if cross is None else cross + term
            mass = t if mass is None else mass + t
        cm_ref[0, 8 * c : 8 * c + 8, :] = jnp.broadcast_to(
            jnp.sum(cross, axis=1, keepdims=True), (8, 128)
        )
        cm_ref[1, 8 * c : 8 * c + 8, :] = jnp.broadcast_to(
            jnp.sum(mass, axis=1, keepdims=True), (8, 128)
        )

    @pl.loop(0, 4)
    def _(c):
        @pl.loop(0, 2)
        def _(h):
            t = c * 4 + h * 2
            dot_into(s1_ref, k_ref, w_ref, t + 1)
            exp_from(s0_ref, e_ref, top_ref, sum_ref, thr_ref, t)
            dot_into(s0_ref, k_ref, w_ref, jnp.minimum(t + 2, 15))
            exp_from(s1_ref, e_ref, top_ref, sum_ref, thr_ref, t + 1)

        stats_out(c)

        @pl.when(c >= 1)
        def _():
            middle(c - 1)

        @pl.when(c >= 2)
        def _():
            head_sum(c - 2)

    for k in range(2):
        n = (3 * 32, 3)[k]
        ref = (iq_ref, iw_ref)[k]
        pltpu.make_async_remote_copy(
            ref.at[pl.ds(0, 3)], ref.at[pl.ds(0, 3)], ix_send.at[k], ix_recv.at[k],
            device_id=x_peer(1), device_id_type=MESH,
        ).wait_recv()
    copies[3].wait()
    for k in range(4):
        w = pltpu.roll(iw_ref[k].astype(f32), lax.rem(128 - 32 * x, 128), 1)
        for q in range(32):
            wc_ref[k * 512 + q * 16 : k * 512 + q * 16 + 16, :] = jnp.broadcast_to(
                w[:, q : q + 1], (16, 128)
            )

    def logits_block(n):
        keys = ik_ref[pl.ds(pl.multiple_of(n * 256, 256), 256), :]
        s0_ref[...] = lax.dot_general(
            iq_ref[...].reshape(2048, 128), keys, (((1,), (1,)), ((), ())),
            preferred_element_type=f32,
        )
        for q in range(32):
            acc = [None, None]
            for k in range(4):
                for h in range(2):
                    r = k * 512 + q * 16 + h * 8
                    w = wc_ref[r : r + 8, :]
                    for j in range(2):
                        v = w * jnp.maximum(s0_ref[r : r + 8, j * 128 : (j + 1) * 128], 0.0)
                        acc[j] = v if acc[j] is None else acc[j] + v
            for j in range(2):
                lg_ref[q : q + 1, pl.ds(pl.multiple_of(n * 256 + j * 128, 128), 128)] = jnp.sum(
                    acc[j], axis=0, keepdims=True
                )

    @pl.loop(0, 4)
    def _(n):
        logits_block(n)

    middle(3)

    @pl.loop(4, 8)
    def _(n):
        logits_block(n)

    head_sum(2)

    cols = []
    lane = lax.broadcasted_iota(jnp.int32, (8, KL), 1)
    for c in range(4):
        rows = slice(8 * c, 8 * c + 8)
        ok = lane <= jnp.broadcast_to(pc_ref[rows, 0:1], (8, KL))
        v = jnp.where(ok, lg_ref[rows, :], NEG)
        top = jnp.max(v, axis=1, keepdims=True)
        total = jnp.sum(jnp.where(ok, jnp.exp(v - top), 0.0), axis=1, keepdims=True)
        cols.append(lse_of(top, total))
    a_start(4, jnp.broadcast_to(as_row(jnp.concatenate(cols, axis=0)), (8, 128)))

    head_sum(3)
    middle(4)
    for c in range(4):
        own_rows(c)
    spread = merge_lse(b_done(4))
    value = as_row(cm_ref[0]) + spread * as_row(cm_ref[1])
    a_start(5, value)
    b_start(5, jnp.sum(a_done(5), axis=0))
    div_ref[...] = jnp.sum(b_done(5), axis=0)

    for k in range(2):
        ref = (iq_ref, iw_ref)[k]
        pltpu.make_async_remote_copy(
            ref.at[pl.ds(0, 3)], ref.at[pl.ds(0, 3)], ix_send.at[k], ix_recv.at[k],
            device_id=x_peer(1), device_id_type=MESH,
        ).wait_send()
    for e in range(NE):
        seven(ab_ref, e, a_send, a_recv).wait_send()
        seven(bb_ref, e, b_send, b_recv).wait_send()
    for c in range(4):
        three(c).wait_send()


def local(query_latent, key_latent, index_query, index_weight, index_key, positions):
    vmem = pl.BlockSpec(memory_space=pltpu.VMEM)
    hbm = pl.BlockSpec(memory_space=pl.ANY)
    bf16 = jnp.bfloat16
    dma = pltpu.SemaphoreType.DMA
    target, divergence = pl.pallas_call(
        kernel,
        out_shape=(
            jax.ShapeDtypeStruct((32, KL), f32),
            jax.ShapeDtypeStruct((8, 128), f32),
        ),
        in_specs=[pl.BlockSpec(memory_space=pltpu.SMEM), vmem, hbm, hbm, hbm, hbm, hbm],
        out_specs=(vmem, vmem),
        scratch_shapes=[
            pltpu.VMEM((32, 576, 128), bf16),
            pltpu.VMEM((576, KL), bf16),
            pltpu.VMEM((KL, 576), bf16),
            pltpu.VMEM((4, 576, 1024), bf16),
            pltpu.VMEM((KL, 256), f32),
            pltpu.VMEM((KL, 256), f32),
            pltpu.VMEM((32, KL, 128), f32),
            pltpu.VMEM((32, 128), f32),
            pltpu.VMEM((32, 128), f32),
            pltpu.VMEM((4, 8, 128), jnp.int32),
            pltpu.VMEM((4, 32, 16, 128), bf16),
            pltpu.VMEM((4, 16, 128), bf16),
            pltpu.VMEM((KL, 128), bf16),
            pltpu.VMEM((2048, 128), f32),
            pltpu.VMEM((32, KL), f32),
            pltpu.VMEM((512, 128), f32),
            pltpu.VMEM((4, 128, 512), f32),
            pltpu.VMEM((4, 4, 32, 512), f32),
            pltpu.VMEM((NE, 8, 8, 128), f32),
            pltpu.VMEM((NE, 8, 8, 128), f32),
            pltpu.VMEM((8, 128), f32),
            pltpu.VMEM((32, 128), jnp.int32),
            pltpu.VMEM((2, 32, 128), f32),
            dma((4,)), dma((2,)), dma((2,)), dma((2,)),
            dma((NE,)), dma((NE,)), dma((NE,)), dma((NE,)), dma((4,)), dma((4,)),
        ],
        compiler_params=pltpu.CompilerParams(
            collective_id=0, has_side_effects=True, vmem_limit_bytes=66_000_000
        ),
    )(
        positions,
        positions.reshape(1, 128),
        query_latent.transpose(1, 2, 0),
        key_latent.T,
        index_query,
        index_weight.T,
        index_key,
    )
    return target, divergence[0, :32]


def solution(mesh):
    finer = Mesh(
        mesh.devices.reshape(8, 4, 2, mesh.shape["head"]), ("z", "y", "c", "x")
    )
    return jax.shard_map(
        local,
        mesh=finer,
        in_specs=(
            P(None, "x", None),
            P(CTX, None),
            P(None, "x", None),
            P(None, "x"),
            P(CTX, None),
            P(),
        ),
        out_specs=(P("x", CTX), P("x")),
        check_vma=False,
    )
```

```python
import jax
import jax.numpy as jnp
from jax import lax
from jax.experimental import pallas as pl
from jax.experimental.pallas import tpu as pltpu
from jax.sharding import Mesh
from jax.sharding import PartitionSpec as P

H = 128
CTX = ("z", "y", "c")
NEG = -1e30
MESH = pl.DeviceIdType.MESH
f32 = jnp.float32
KL = 2048
QK = 576
PIECE = 256
NE = 6


def build_weights(q_ref, w_ref, t):
    group = (lax.broadcasted_iota(jnp.int32, (QK, 128), 1) // 8) % 4
    c = t // 4
    for j in range(2):
        i = (t % 4) * 2 + j
        out = None
        for g in range(4):
            r = pltpu.roll(q_ref[4 * i + g], lax.rem(8 * (g - c) + 128, 128), 1)
            out = r if out is None else jnp.where(group == g, r, out)
        w_ref[:, j * 128 : (j + 1) * 128] = out


def score_step(new_ref, old_ref, k_ref, w_ref, e_ref, top_ref, sum_ref, thr_ref, t, new=True,
               old=True, before=None):
    nt = t + 1
    biggest = [[None] * 2 for _ in range(2)]
    total = [[None] * 4 for _ in range(2)]
    if new:
        th = thr_ref[nt // 4]
        w = w_ref[...]
    if old:
        tops = [jnp.broadcast_to(top_ref[pl.ds(2 * t + j, 1), :], (8, 128)) for j in range(2)]
    for p in range(KL // PIECE):
        if before is not None:
            before(p)
        rows = slice(p * PIECE, (p + 1) * PIECE)
        if new:
            r = lax.dot_general(
                k_ref[rows, :], w, (((1,), (0,)), ((), ())), preferred_element_type=f32
            )
            for k in range(PIECE // 8):
                at = p * PIECE + 8 * k
                m = th >= at
                for j in range(2):
                    v = jnp.where(m, r[8 * k : 8 * k + 8, j * 128 : (j + 1) * 128], NEG)
                    new_ref[at : at + 8, j * 128 : (j + 1) * 128] = v
                    a = k % 2
                    biggest[j][a] = v if biggest[j][a] is None else jnp.maximum(biggest[j][a], v)
        if old:
            for k in range(PIECE // 8):
                at = p * PIECE + 8 * k
                for j in range(2):
                    v = jnp.exp(old_ref[at : at + 8, j * 128 : (j + 1) * 128] - tops[j])
                    e_ref[t // 4, at // 8, (t % 4) * 2 + j] = v
                    a = k % 4
                    total[j][a] = v if total[j][a] is None else total[j][a] + v
    for j in range(2):
        if new:
            m = jnp.max(jnp.maximum(biggest[j][0], biggest[j][1]), axis=0, keepdims=True)
            top_ref[pl.ds(2 * nt + j, 1), :] = jnp.maximum(m, 0.5 * NEG)
        if old:
            m = (total[j][0] + total[j][1]) + (total[j][2] + total[j][3])
            sum_ref[pl.ds(2 * t + j, 1), :] = jnp.sum(m, axis=0, keepdims=True)


def lse_of(top, total):
    some = total > 0
    return jnp.where(some, top + jnp.log(jnp.where(some, total, 1.0)), NEG)


def merge_lse(v):
    m = jnp.max(v, axis=0)
    return m + jnp.log(jnp.sum(jnp.exp(v - m[None]), axis=0))


def as_row(column):
    n = column.shape[0]
    row = lax.broadcasted_iota(jnp.int32, (n, 128), 0)
    lane = lax.broadcasted_iota(jnp.int32, (n, 128), 1)
    return jnp.sum(jnp.where(row == lane, column, 0.0), axis=0, keepdims=True)


def kernel(
    pos_s, pos_v, q_hbm, k_hbm, iq_hbm, iw_hbm, ik_hbm,
    tgt_ref, div_ref,
    q_ref, kt_ref, k_ref, w0_ref, w1_ref, s0_ref, s1_ref, e_ref, top_ref, sum_ref, thr_ref,
    iq_ref, iw_ref, ik_ref, wc_ref, lg_ref, u_ref, part_ref, got_ref,
    ab_ref, bb_ref, l_ref, pc_ref, cm_ref, ikt_ref, f_ref,
    in_sem, ix_sem, ix_send, ix_recv, a_send, a_recv, b_send, b_recv, r_send, r_recv,
):
    z, y, c0, x = (lax.axis_index(n) for n in ("z", "y", "c", "x"))
    me_a = y * 2 + c0
    base = ((z * 4 + y) * 2 + c0) * KL

    def x_peer(d):
        return {"z": z, "y": y, "c": c0, "x": lax.rem(x + d, 4)}

    def a_peer(d):
        p = lax.rem(me_a + d, 8)
        return {"z": z, "y": p // 2, "c": lax.rem(p, 2), "x": x}

    def b_peer(d):
        return {"z": lax.rem(z + d, 8), "y": y, "c": c0, "x": x}

    k_in = [
        pltpu.make_async_copy(
            k_hbm.at[:, pl.ds(n * 512, 512)], kt_ref.at[:, pl.ds(n * 512, 512)], in_sem.at[n]
        )
        for n in range(4)
    ]
    q_in = [
        pltpu.make_async_copy(
            q_hbm.at[pl.ds(n * 8, 8)], q_ref.at[pl.ds(n * 8, 8)], in_sem.at[4 + n]
        )
        for n in range(4)
    ]
    ik_in = pltpu.make_async_copy(ik_hbm, ik_ref, in_sem.at[8])
    q_in[0].start()
    for cp in k_in:
        cp.start()
    for cp in q_in[1:]:
        cp.start()
    ik_in.start()
    own_iq = pltpu.make_async_copy(
        iq_hbm.at[pl.ds(x * 4, 4)], iq_ref.at[:, x], ix_sem.at[0]
    )
    own_iw = pltpu.make_async_copy(iw_hbm, iw_ref.at[x], ix_sem.at[1])
    own_iq.start()
    own_iw.start()

    barrier = pltpu.get_barrier_semaphore()
    for d in range(1, 4):
        pl.semaphore_signal(barrier, inc=1, device_id=x_peer(d), device_id_type=MESH)
    for d in range(1, 8):
        pl.semaphore_signal(barrier, inc=1, device_id=a_peer(d), device_id_type=MESH)
        pl.semaphore_signal(barrier, inc=1, device_id=b_peer(d), device_id_type=MESH)

    group = (lax.broadcasted_iota(jnp.int32, (8, 128), 1) // 8) % 4
    sub = lax.broadcasted_iota(jnp.int32, (8, 128), 0)
    pos8 = jnp.broadcast_to(pos_v[...], (8, 128))
    for c in range(4):
        th = pos8
        for g in range(4):
            if g != c:
                th = jnp.where(group == g, pltpu.roll(pos8, (8 * (g - c)) % 128, 1), th)
        thr_ref[c] = th - base - sub
    for q in range(32):
        pc_ref[q : q + 1, :] = jnp.full((1, 128), pos_s[x * 32 + q] - base, jnp.int32)

    q_in[0].wait()
    build_weights(q_ref, w0_ref, 0)

    def key_block(p):
        if p % (512 // PIECE) == 0:
            k_in[p * PIECE // 512].wait()
        for n in range(PIECE // 128):
            at = p * PIECE + n * 128
            k_ref[at : at + 128, :] = kt_ref[:, at : at + 128].T

    score_step(
        s1_ref, s0_ref, k_ref, w0_ref, e_ref, top_ref, sum_ref, thr_ref, -1, old=False,
        before=key_block,
    )
    for cp in q_in[1:]:
        cp.wait()
    build_weights(q_ref, w1_ref, 1)

    pl.semaphore_wait(barrier, 17)
    own_iq.wait()
    own_iw.wait()

    def ix_copies(d):
        peer = x_peer(d)
        to = lax.rem(x + d, 4)
        return [
            pltpu.make_async_remote_copy(
                iq_hbm.at[pl.ds(to * 4, 4)], iq_ref.at[:, x],
                ix_send.at[0], ix_recv.at[0], device_id=peer, device_id_type=MESH,
            ),
            pltpu.make_async_remote_copy(
                iw_hbm, iw_ref.at[x],
                ix_send.at[1], ix_recv.at[1], device_id=peer, device_id_type=MESH,
            ),
        ]

    for d in range(1, 4):
        for cp in ix_copies(d):
            cp.start()

    def ix_all():
        return [
            pltpu.make_async_remote_copy(
                ref, ref, ix_send.at[k], ix_recv.at[k],
                device_id=x_peer(1), device_id_type=MESH,
            )
            for k, ref in enumerate((iq_ref.at[:, pl.ds(0, 3)], iw_ref.at[pl.ds(0, 3)]))
        ]

    def exchange_start(buf, me, e, value, send, recv, peer):
        buf[e, me] = value
        for d in range(1, 8):
            pltpu.make_async_remote_copy(
                buf.at[e, me], buf.at[e, me], send.at[e], recv.at[e],
                device_id=peer(d), device_id_type=MESH,
            ).start()

    def seven(buf, e, send, recv):
        return pltpu.make_async_remote_copy(
            buf.at[e, pl.ds(0, 7)], buf.at[e, pl.ds(0, 7)], send.at[e], recv.at[e],
            device_id=x_peer(1), device_id_type=MESH,
        )

    def a_start(e, value):
        exchange_start(ab_ref, me_a, e, value, a_send, a_recv, a_peer)

    def a_done(e):
        seven(ab_ref, e, a_send, a_recv).wait_recv()
        return ab_ref[e]

    def b_start(e, value):
        exchange_start(bb_ref, z, e, value, b_send, b_recv, b_peer)

    def b_done(e):
        seven(bb_ref, e, b_send, b_recv).wait_recv()
        return bb_ref[e]

    def stats_out(c):
        rows = pl.ds(pl.multiple_of(c * 8, 8), 8)
        a_start(c, lse_of(top_ref[rows, :], sum_ref[rows, :]))

    def middle(c):
        b_start(c, merge_lse(a_done(c)))

    def head_sum(c):
        lse = merge_lse(b_done(c))
        rows = pl.ds(pl.multiple_of(c * 8, 8), 8)
        l_ref[...] = jnp.exp(top_ref[rows, :] - lse) * (1.0 / H)
        coef = [jnp.broadcast_to(l_ref[i : i + 1, :], (8, 128)) for i in range(8)]

        @pl.loop(0, 8)
        def _(b):
            for k in range(32):
                at = b * 32 + k
                s = e_ref[c, at, 0] * coef[0]
                for i in range(1, 8):
                    s = s + e_ref[c, at, i] * coef[i]
                u_ref[at] = s

        for n in range(16):
            v = u_ref[n * 16 : n * 16 + 16].reshape(128, 128).T
            for k in range(4):
                r = [v[32 * k + 8 * g : 32 * k + 8 * g + 8, :] for g in range(4)]
                part_ref[c, k, :, n * 128 : (n + 1) * 128] = (r[0] + r[1]) + (r[2] + r[3])
        for d in range(1, 4):
            to = lax.rem(x + d, 4)
            pltpu.make_async_remote_copy(
                part_ref.at[c, to], got_ref.at[c, x],
                r_send.at[c], r_recv.at[c], device_id=x_peer(d), device_id_type=MESH,
            ).start()

    def three(c):
        return pltpu.make_async_remote_copy(
            got_ref.at[c, pl.ds(0, 3)], got_ref.at[c, pl.ds(0, 3)],
            r_send.at[c], r_recv.at[c], device_id=x_peer(1), device_id_type=MESH,
        )

    def own_rows(c):
        three(c).wait_recv()
        got_ref[c, x] = part_ref[c, x]
        rows = slice(8 * c, 8 * c + 8)
        cross = [None] * 4
        mass = [None] * 4
        for n in range(16):
            at = slice(n * 128, (n + 1) * 128)
            t = (got_ref[c, 0, :, at] + got_ref[c, 1, :, at]) + (
                got_ref[c, 2, :, at] + got_ref[c, 3, :, at]
            )
            tgt_ref[rows, at] = t
            positive = t > 0
            log = jnp.log(jnp.where(positive, t, 1.0))
            term = jnp.where(positive, t * log, 0.0) - t * lg_ref[rows, at]
            a = n % 4
            cross[a] = term if cross[a] is None else cross[a] + term
            mass[a] = t if mass[a] is None else mass[a] + t
        cross = (cross[0] + cross[1]) + (cross[2] + cross[3])
        mass = (mass[0] + mass[1]) + (mass[2] + mass[3])
        cm_ref[0, 8 * c : 8 * c + 8, :] = jnp.broadcast_to(
            jnp.sum(cross, axis=1, keepdims=True), (8, 128)
        )
        cm_ref[1, 8 * c : 8 * c + 8, :] = jnp.broadcast_to(
            jnp.sum(mass, axis=1, keepdims=True), (8, 128)
        )

    @pl.loop(0, 4)
    def _(c):
        @pl.loop(0, 2)
        def _(h):
            t = c * 4 + h * 2
            build_weights(q_ref, w0_ref, jnp.minimum(t + 2, 15))
            score_step(s0_ref, s1_ref, k_ref, w1_ref, e_ref, top_ref, sum_ref, thr_ref, t)

            @pl.when(t < 14)
            def _():
                build_weights(q_ref, w1_ref, jnp.minimum(t + 3, 15))
                score_step(s1_ref, s0_ref, k_ref, w0_ref, e_ref, top_ref, sum_ref, thr_ref, t + 1)

            @pl.when(t == 14)
            def _():
                score_step(
                    s1_ref, s0_ref, k_ref, w0_ref, e_ref, top_ref, sum_ref, thr_ref, t + 1,
                    new=False,
                )

        stats_out(c)

        @pl.when(c >= 1)
        def _():
            middle(c - 1)

        @pl.when(c >= 2)
        def _():
            head_sum(c - 2)

    for cp in ix_all():
        cp.wait_recv()
    ik_in.wait()
    for n in range(KL // 128):
        ikt_ref[:, n * 128 : (n + 1) * 128] = ik_ref[n * 128 : (n + 1) * 128, :].T
    for k in range(4):
        w = pltpu.roll(iw_ref[k].astype(f32), lax.rem(128 - 32 * x, 128), 1)
        for q in range(32):
            wc_ref[q // 8, k, q % 8] = jnp.broadcast_to(w[:, q : q + 1], (16, 128))

    def logits_block(n, s):
        at = pl.ds(pl.multiple_of(n * 256, 256), 256)
        keys = ikt_ref[:, at]
        for b in range(4):
            r = lax.dot_general(
                iq_ref[b].reshape(512, 128), keys, (((1,), (0,)), ((), ())),
                preferred_element_type=f32,
            )
            for q in range(8):
                acc = [None, None]
                for k in range(4):
                    for h in range(2):
                        o = k * 128 + q * 16 + h * 8
                        w = wc_ref[b, k, q, h * 8 : h * 8 + 8, :]
                        for j in range(2):
                            v = w * jnp.maximum(r[o : o + 8, j * 128 : (j + 1) * 128], 0.0)
                            acc[j] = v if acc[j] is None else acc[j] + v
                for j in range(2):
                    f_ref[s, b, j, q * 8 : q * 8 + 8, :] = acc[j]
        for b in range(4):
            for j in range(2):
                v = f_ref[s, b, j, pl.ds(0, 8, stride=8), :]
                for i in range(1, 8):
                    v = v + f_ref[s, b, j, pl.ds(i, 8, stride=8), :]
                lg_ref[8 * b : 8 * b + 8, pl.ds(pl.multiple_of(n * 256 + j * 128, 128), 128)] = v

    @pl.loop(0, 2)
    def _(n):
        logits_block(n * 2, 0)
        logits_block(n * 2 + 1, 1)

    middle(3)

    @pl.loop(2, 4)
    def _(n):
        logits_block(n * 2, 0)
        logits_block(n * 2 + 1, 1)

    head_sum(2)

    cols = []
    lane = lax.broadcasted_iota(jnp.int32, (8, KL), 1)
    for c in range(4):
        rows = slice(8 * c, 8 * c + 8)
        ok = lane <= jnp.broadcast_to(pc_ref[rows, 0:1], (8, KL))
        v = jnp.where(ok, lg_ref[rows, :], NEG)
        top = jnp.max(v, axis=1, keepdims=True)
        total = jnp.sum(jnp.where(ok, jnp.exp(v - top), 0.0), axis=1, keepdims=True)
        cols.append(lse_of(top, total))
    a_start(4, jnp.broadcast_to(as_row(jnp.concatenate(cols, axis=0)), (8, 128)))

    head_sum(3)
    middle(4)
    for c in range(4):
        own_rows(c)
    spread = merge_lse(b_done(4))
    value = as_row(cm_ref[0]) + spread * as_row(cm_ref[1])
    a_start(5, value)
    b_start(5, jnp.sum(a_done(5), axis=0))
    div_ref[...] = jnp.sum(b_done(5), axis=0)

    for cp in ix_all():
        cp.wait_send()
    for e in range(NE):
        seven(ab_ref, e, a_send, a_recv).wait_send()
        seven(bb_ref, e, b_send, b_recv).wait_send()
    for c in range(4):
        three(c).wait_send()


def local(query_latent, key_latent, index_query, index_weight, index_key, positions):
    vmem = pl.BlockSpec(memory_space=pltpu.VMEM)
    hbm = pl.BlockSpec(memory_space=pl.ANY)
    bf16 = jnp.bfloat16
    dma = pltpu.SemaphoreType.DMA
    target, divergence = pl.pallas_call(
        kernel,
        out_shape=(
            jax.ShapeDtypeStruct((32, KL), f32),
            jax.ShapeDtypeStruct((8, 128), f32),
        ),
        in_specs=[pl.BlockSpec(memory_space=pltpu.SMEM), vmem, hbm, hbm, hbm, hbm, hbm],
        out_specs=(vmem, vmem),
        scratch_shapes=[
            pltpu.VMEM((32, 576, 128), bf16),
            pltpu.VMEM((576, KL), bf16),
            pltpu.VMEM((KL, 576), bf16),
            pltpu.VMEM((QK, 256), bf16),
            pltpu.VMEM((QK, 256), bf16),
            pltpu.VMEM((KL, 256), f32),
            pltpu.VMEM((KL, 256), f32),
            pltpu.VMEM((4, KL // 8, 8, 8, 128), f32),
            pltpu.VMEM((32, 128), f32),
            pltpu.VMEM((32, 128), f32),
            pltpu.VMEM((4, 8, 128), jnp.int32),
            pltpu.VMEM((4, 4, 8, 16, 128), bf16),
            pltpu.VMEM((4, 16, 128), bf16),
            pltpu.VMEM((KL, 128), bf16),
            pltpu.VMEM((4, 4, 8, 16, 128), f32),
            pltpu.VMEM((32, KL), f32),
            pltpu.VMEM((KL // 8, 8, 128), f32),
            pltpu.VMEM((4, 4, 8, KL), f32),
            pltpu.VMEM((4, 4, 8, KL), f32),
            pltpu.VMEM((NE, 8, 8, 128), f32),
            pltpu.VMEM((NE, 8, 8, 128), f32),
            pltpu.VMEM((8, 128), f32),
            pltpu.VMEM((32, 128), jnp.int32),
            pltpu.VMEM((2, 32, 128), f32),
            pltpu.VMEM((128, KL), bf16),
            pltpu.VMEM((2, 4, 2, 64, 128), f32),
            dma((9,)), dma((2,)), dma((2,)), dma((2,)),
            dma((NE,)), dma((NE,)), dma((NE,)), dma((NE,)), dma((4,)), dma((4,)),
        ],
        compiler_params=pltpu.CompilerParams(
            collective_id=0, has_side_effects=True, vmem_limit_bytes=66_000_000
        ),
    )(
        positions,
        positions.reshape(1, 128),
        query_latent.transpose(1, 2, 0),
        key_latent.T,
        index_query.reshape(16, 8, 16, 128),
        index_weight.T,
        index_key,
    )
    return target, divergence[0, :32]


def solution(mesh):
    finer = Mesh(
        mesh.devices.reshape(8, 4, 2, mesh.shape["head"]), ("z", "y", "c", "x")
    )
    return jax.shard_map(
        local,
        mesh=finer,
        in_specs=(
            P(None, "x", None),
            P(CTX, None),
            P(None, "x", None),
            P(None, "x"),
            P(CTX, None),
            P(),
        ),
        out_specs=(P("x", CTX), P("x")),
        check_vma=False,
    )
```

```python
import functools

import jax
import jax.numpy as jnp
from jax import lax
from jax.experimental import pallas as pl
from jax.experimental.pallas import tpu as pltpu
from jax.sharding import Mesh
from jax.sharding import PartitionSpec as P

H = 128
CTX = ("z", "y", "c")
NEG = -1e30
MESH = pl.DeviceIdType.MESH
f32 = jnp.float32
KL = 2048
QK = 576
PIECE = 256
NE = 6


def build_weights(q_ref, w_ref, t):
    group = (lax.broadcasted_iota(jnp.int32, (QK, 128), 1) // 8) % 4
    c = t // 4
    for j in range(2):
        i = (t % 4) * 2 + j
        out = None
        for g in range(4):
            r = pltpu.roll(q_ref[4 * i + g], lax.rem(8 * (g - c) + 128, 128), 1)
            out = r if out is None else jnp.where(group == g, r, out)
        w_ref[:, j * 128 : (j + 1) * 128] = out


def score_step(new_ref, old_ref, k_ref, w_ref, e_ref, top_ref, sum_ref, thr_ref, t, new=True,
               old=True, before=None):
    nt = t + 1
    biggest = [[None] * 8 for _ in range(2)]
    total = [None] * 2
    if new:
        th = thr_ref[nt // 4]
        w = w_ref[...]
    if old:
        tops = [jnp.broadcast_to(top_ref[pl.ds(2 * t + j, 1), :], (8, 128)) for j in range(2)]
    for p in range(KL // PIECE):
        if before is not None:
            before(p)
        rows = slice(p * PIECE, (p + 1) * PIECE)
        if new:
            r = lax.dot_general(
                k_ref[rows, :], w, (((1,), (0,)), ((), ())), preferred_element_type=f32
            )
            for k in range(PIECE // 8):
                at = p * PIECE + 8 * k
                m = th >= at
                for j in range(2):
                    v = jnp.where(m, r[8 * k : 8 * k + 8, j * 128 : (j + 1) * 128], NEG)
                    new_ref[at : at + 8, j * 128 : (j + 1) * 128] = v
                    a = k % 8
                    biggest[j][a] = v if biggest[j][a] is None else jnp.maximum(biggest[j][a], v)
        if old:
            for k in range(PIECE // 8):
                at = p * PIECE + 8 * k
                for j in range(2):
                    v = jnp.exp(old_ref[at : at + 8, j * 128 : (j + 1) * 128] - tops[j])
                    e_ref[t // 4, at // 8, (t % 4) * 2 + j] = v
                    total[j] = v if total[j] is None else total[j] + v
    for j in range(2):
        if new:
            m = jnp.max(functools.reduce(jnp.maximum, biggest[j]), axis=0, keepdims=True)
            top_ref[pl.ds(2 * nt + j, 1), :] = jnp.maximum(m, 0.5 * NEG)
        if old:
            sum_ref[pl.ds(2 * t + j, 1), :] = jnp.sum(total[j], axis=0, keepdims=True)


def lse_of(top, total):
    some = total > 0
    return jnp.where(some, top + jnp.log(jnp.where(some, total, 1.0)), NEG)


def merge_lse(v):
    m = jnp.max(v, axis=0)
    return m + jnp.log(jnp.sum(jnp.exp(v - m[None]), axis=0))


def as_row(column):
    n = column.shape[0]
    row = lax.broadcasted_iota(jnp.int32, (n, 128), 0)
    lane = lax.broadcasted_iota(jnp.int32, (n, 128), 1)
    return jnp.sum(jnp.where(row == lane, column, 0.0), axis=0, keepdims=True)


def kernel(
    pos_s, pos_v, q_hbm, k_hbm, iq_hbm, iw_hbm, ik_hbm,
    tgt_ref, div_ref,
    q_ref, kt_ref, k_ref, w0_ref, w1_ref, s0_ref, s1_ref, e_ref, top_ref, sum_ref, thr_ref,
    iq_ref, iw_ref, ik_ref, wc_ref, lg_ref, u_ref, part_ref, got_ref,
    ab_ref, bb_ref, l_ref, pc_ref, cm_ref, ikt_ref, f_ref,
    in_sem, ix_sem, ix_send, ix_recv, a_send, a_recv, b_send, b_recv, r_send, r_recv,
):
    z, y, c0, x = (lax.axis_index(n) for n in ("z", "y", "c", "x"))
    me_a = y * 2 + c0
    base = ((z * 4 + y) * 2 + c0) * KL

    def x_peer(d):
        return {"z": z, "y": y, "c": c0, "x": lax.rem(x + d, 4)}

    def a_peer(d):
        p = lax.rem(me_a + d, 8)
        return {"z": z, "y": p // 2, "c": lax.rem(p, 2), "x": x}

    def b_peer(d):
        return {"z": lax.rem(z + d, 8), "y": y, "c": c0, "x": x}

    k_in = [
        pltpu.make_async_copy(
            k_hbm.at[:, pl.ds(n * 512, 512)], kt_ref.at[:, pl.ds(n * 512, 512)], in_sem.at[n]
        )
        for n in range(4)
    ]
    q_in = [
        pltpu.make_async_copy(
            q_hbm.at[pl.ds(n * 8, 8)], q_ref.at[pl.ds(n * 8, 8)], in_sem.at[4 + n]
        )
        for n in range(4)
    ]
    ik_in = pltpu.make_async_copy(ik_hbm, ik_ref, in_sem.at[8])
    q_in[0].start()
    for cp in k_in:
        cp.start()
    own_iq = pltpu.make_async_copy(
        iq_hbm.at[pl.ds(x * 4, 4)], iq_ref.at[:, x], ix_sem.at[0]
    )
    own_iw = pltpu.make_async_copy(iw_hbm, iw_ref.at[x], ix_sem.at[1])
    own_iq.start()
    own_iw.start()

    barrier = pltpu.get_barrier_semaphore()
    for d in range(1, 4):
        pl.semaphore_signal(barrier, inc=1, device_id=x_peer(d), device_id_type=MESH)
    for d in range(1, 8):
        pl.semaphore_signal(barrier, inc=1, device_id=a_peer(d), device_id_type=MESH)
        pl.semaphore_signal(barrier, inc=1, device_id=b_peer(d), device_id_type=MESH)

    group = (lax.broadcasted_iota(jnp.int32, (8, 128), 1) // 8) % 4
    sub = lax.broadcasted_iota(jnp.int32, (8, 128), 0)
    pos8 = jnp.broadcast_to(pos_v[...], (8, 128))
    for c in range(4):
        th = pos8
        for g in range(4):
            if g != c:
                th = jnp.where(group == g, pltpu.roll(pos8, (8 * (g - c)) % 128, 1), th)
        thr_ref[c] = th - base - sub
    for q in range(32):
        pc_ref[q : q + 1, :] = jnp.full((1, 128), pos_s[x * 32 + q] - base, jnp.int32)

    q_in[0].wait()
    build_weights(q_ref, w0_ref, 0)

    def key_block(p):
        if p % (512 // PIECE) == 0:
            k_in[p * PIECE // 512].wait()
        if p == 0:
            for cp in q_in[1:]:
                cp.start()
            ik_in.start()
        for n in range(PIECE // 128):
            at = p * PIECE + n * 128
            k_ref[at : at + 128, :] = kt_ref[:, at : at + 128].T

    score_step(
        s1_ref, s0_ref, k_ref, w0_ref, e_ref, top_ref, sum_ref, thr_ref, -1, old=False,
        before=key_block,
    )
    for cp in q_in[1:]:
        cp.wait()
    build_weights(q_ref, w1_ref, 1)

    pl.semaphore_wait(barrier, 17)
    own_iq.wait()
    own_iw.wait()

    def ix_copies(d):
        peer = x_peer(d)
        to = lax.rem(x + d, 4)
        return [
            pltpu.make_async_remote_copy(
                iq_hbm.at[pl.ds(to * 4, 4)], iq_ref.at[:, x],
                ix_send.at[0], ix_recv.at[0], device_id=peer, device_id_type=MESH,
            ),
            pltpu.make_async_remote_copy(
                iw_hbm, iw_ref.at[x],
                ix_send.at[1], ix_recv.at[1], device_id=peer, device_id_type=MESH,
            ),
        ]

    for d in range(1, 4):
        for cp in ix_copies(d):
            cp.start()

    def ix_all():
        return [
            pltpu.make_async_remote_copy(
                ref, ref, ix_send.at[k], ix_recv.at[k],
                device_id=x_peer(1), device_id_type=MESH,
            )
            for k, ref in enumerate((iq_ref.at[:, pl.ds(0, 3)], iw_ref.at[pl.ds(0, 3)]))
        ]

    def exchange_start(buf, me, e, value, send, recv, peer):
        buf[e, me] = value
        for d in range(1, 8):
            pltpu.make_async_remote_copy(
                buf.at[e, me], buf.at[e, me], send.at[e], recv.at[e],
                device_id=peer(d), device_id_type=MESH,
            ).start()

    def seven(buf, e, send, recv):
        return pltpu.make_async_remote_copy(
            buf.at[e, pl.ds(0, 7)], buf.at[e, pl.ds(0, 7)], send.at[e], recv.at[e],
            device_id=x_peer(1), device_id_type=MESH,
        )

    def a_start(e, value):
        exchange_start(ab_ref, me_a, e, value, a_send, a_recv, a_peer)

    def a_done(e):
        seven(ab_ref, e, a_send, a_recv).wait_recv()
        return ab_ref[e]

    def b_start(e, value):
        exchange_start(bb_ref, z, e, value, b_send, b_recv, b_peer)

    def b_done(e):
        seven(bb_ref, e, b_send, b_recv).wait_recv()
        return bb_ref[e]

    def stats_out(c):
        rows = pl.ds(pl.multiple_of(c * 8, 8), 8)
        a_start(c, lse_of(top_ref[rows, :], sum_ref[rows, :]))

    def middle(c):
        b_start(c, merge_lse(a_done(c)))

    def head_sum(c):
        lse = merge_lse(b_done(c))
        rows = pl.ds(pl.multiple_of(c * 8, 8), 8)
        l_ref[...] = jnp.exp(top_ref[rows, :] - lse) * (1.0 / H)
        coef = [jnp.broadcast_to(l_ref[i : i + 1, :], (8, 128)) for i in range(8)]

        @pl.loop(0, 8)
        def _(b):
            for k in range(32):
                at = b * 32 + k
                s = e_ref[c, at, 0] * coef[0]
                for i in range(1, 8):
                    s = s + e_ref[c, at, i] * coef[i]
                u_ref[at] = s

        for n in range(16):
            v = u_ref[n * 16 : n * 16 + 16].reshape(128, 128).T
            for k in range(4):
                r = [v[32 * k + 8 * g : 32 * k + 8 * g + 8, :] for g in range(4)]
                part_ref[c, k, :, n * 128 : (n + 1) * 128] = (r[0] + r[1]) + (r[2] + r[3])
        for d in range(1, 4):
            to = lax.rem(x + d, 4)
            pltpu.make_async_remote_copy(
                part_ref.at[c, to], got_ref.at[c, x],
                r_send.at[c], r_recv.at[c], device_id=x_peer(d), device_id_type=MESH,
            ).start()

    def three(c):
        return pltpu.make_async_remote_copy(
            got_ref.at[c, pl.ds(0, 3)], got_ref.at[c, pl.ds(0, 3)],
            r_send.at[c], r_recv.at[c], device_id=x_peer(1), device_id_type=MESH,
        )

    def own_rows(c):
        three(c).wait_recv()
        got_ref[c, x] = part_ref[c, x]
        rows = slice(8 * c, 8 * c + 8)
        cross = [None] * 4
        mass = [None] * 4
        for n in range(16):
            at = slice(n * 128, (n + 1) * 128)
            t = (got_ref[c, 0, :, at] + got_ref[c, 1, :, at]) + (
                got_ref[c, 2, :, at] + got_ref[c, 3, :, at]
            )
            tgt_ref[rows, at] = t
            positive = t > 0
            log = jnp.log(jnp.where(positive, t, 1.0))
            term = jnp.where(positive, t * log, 0.0) - t * lg_ref[rows, at]
            a = n % 4
            cross[a] = term if cross[a] is None else cross[a] + term
            mass[a] = t if mass[a] is None else mass[a] + t
        cross = (cross[0] + cross[1]) + (cross[2] + cross[3])
        mass = (mass[0] + mass[1]) + (mass[2] + mass[3])
        cm_ref[0, 8 * c : 8 * c + 8, :] = jnp.broadcast_to(
            jnp.sum(cross, axis=1, keepdims=True), (8, 128)
        )
        cm_ref[1, 8 * c : 8 * c + 8, :] = jnp.broadcast_to(
            jnp.sum(mass, axis=1, keepdims=True), (8, 128)
        )

    @pl.loop(0, 4)
    def _(c):
        @pl.loop(0, 2)
        def _(h):
            t = c * 4 + h * 2
            build_weights(q_ref, w0_ref, jnp.minimum(t + 2, 15))
            score_step(s0_ref, s1_ref, k_ref, w1_ref, e_ref, top_ref, sum_ref, thr_ref, t)

            @pl.when(t < 14)
            def _():
                build_weights(q_ref, w1_ref, jnp.minimum(t + 3, 15))
                score_step(s1_ref, s0_ref, k_ref, w0_ref, e_ref, top_ref, sum_ref, thr_ref, t + 1)

            @pl.when(t == 14)
            def _():
                score_step(
                    s1_ref, s0_ref, k_ref, w0_ref, e_ref, top_ref, sum_ref, thr_ref, t + 1,
                    new=False,
                )

        stats_out(c)

        @pl.when(c >= 1)
        def _():
            middle(c - 1)

    head_sum(0)
    head_sum(1)

    for cp in ix_all():
        cp.wait_recv()
    ik_in.wait()
    for n in range(KL // 128):
        ikt_ref[:, n * 128 : (n + 1) * 128] = ik_ref[n * 128 : (n + 1) * 128, :].T
    for k in range(4):
        w = pltpu.roll(iw_ref[k].astype(f32), lax.rem(128 - 32 * x, 128), 1)
        for q in range(32):
            wc_ref[q // 8, k, q % 8] = jnp.broadcast_to(w[:, q : q + 1], (16, 128))

    def logits_block(n, s):
        at = pl.ds(pl.multiple_of(n * 256, 256), 256)
        keys = ikt_ref[:, at]
        for b in range(4):
            r = lax.dot_general(
                iq_ref[b].reshape(512, 128), keys, (((1,), (0,)), ((), ())),
                preferred_element_type=f32,
            )
            for q in range(8):
                acc = [None, None]
                for k in range(4):
                    for h in range(2):
                        o = k * 128 + q * 16 + h * 8
                        w = wc_ref[b, k, q, h * 8 : h * 8 + 8, :]
                        for j in range(2):
                            v = w * jnp.maximum(r[o : o + 8, j * 128 : (j + 1) * 128], 0.0)
                            acc[j] = v if acc[j] is None else acc[j] + v
                for j in range(2):
                    f_ref[s, b, j, q * 8 : q * 8 + 8, :] = acc[j]
        for b in range(4):
            for j in range(2):
                v = f_ref[s, b, j, pl.ds(0, 8, stride=8), :]
                for i in range(1, 8):
                    v = v + f_ref[s, b, j, pl.ds(i, 8, stride=8), :]
                lg_ref[8 * b : 8 * b + 8, pl.ds(pl.multiple_of(n * 256 + j * 128, 128), 128)] = v

    @pl.loop(0, 2)
    def _(n):
        logits_block(n * 2, 0)
        logits_block(n * 2 + 1, 1)

    middle(3)

    @pl.loop(2, 4)
    def _(n):
        logits_block(n * 2, 0)
        logits_block(n * 2 + 1, 1)

    head_sum(2)

    cols = []
    lane = lax.broadcasted_iota(jnp.int32, (8, KL), 1)
    for c in range(4):
        rows = slice(8 * c, 8 * c + 8)
        ok = lane <= jnp.broadcast_to(pc_ref[rows, 0:1], (8, KL))
        v = jnp.where(ok, lg_ref[rows, :], NEG)
        top = jnp.max(v, axis=1, keepdims=True)
        total = jnp.sum(jnp.where(ok, jnp.exp(v - top), 0.0), axis=1, keepdims=True)
        cols.append(lse_of(top, total))
    a_start(4, jnp.broadcast_to(as_row(jnp.concatenate(cols, axis=0)), (8, 128)))

    own_rows(0)
    head_sum(3)
    middle(4)
    for c in range(1, 4):
        own_rows(c)
    spread = merge_lse(b_done(4))
    value = as_row(cm_ref[0]) + spread * as_row(cm_ref[1])
    a_start(5, value)
    b_start(5, jnp.sum(a_done(5), axis=0))
    div_ref[...] = jnp.sum(b_done(5), axis=0)

    for cp in ix_all():
        cp.wait_send()
    for e in range(NE):
        seven(ab_ref, e, a_send, a_recv).wait_send()
        seven(bb_ref, e, b_send, b_recv).wait_send()
    for c in range(4):
        three(c).wait_send()


def results(sum_ref, row_ref, tgt_ref, div_ref):
    tgt_ref[...] = sum_ref[...]
    div_ref[...] = row_ref[0, 0:32]


def local(query_latent, key_latent, index_query, index_weight, index_key, positions):
    vmem = pl.BlockSpec(memory_space=pltpu.VMEM)
    hbm = pl.BlockSpec(memory_space=pl.ANY)
    bf16 = jnp.bfloat16
    dma = pltpu.SemaphoreType.DMA
    target, divergence = pl.pallas_call(
        kernel,
        out_shape=(
            jax.ShapeDtypeStruct((32, KL), f32),
            jax.ShapeDtypeStruct((8, 128), f32),
        ),
        in_specs=[pl.BlockSpec(memory_space=pltpu.SMEM), vmem, hbm, hbm, hbm, hbm, hbm],
        out_specs=(vmem, vmem),
        scratch_shapes=[
            pltpu.VMEM((32, 576, 128), bf16),
            pltpu.VMEM((576, KL), bf16),
            pltpu.VMEM((KL, 576), bf16),
            pltpu.VMEM((QK, 256), bf16),
            pltpu.VMEM((QK, 256), bf16),
            pltpu.VMEM((KL, 256), f32),
            pltpu.VMEM((KL, 256), f32),
            pltpu.VMEM((4, KL // 8, 8, 8, 128), f32),
            pltpu.VMEM((32, 128), f32),
            pltpu.VMEM((32, 128), f32),
            pltpu.VMEM((4, 8, 128), jnp.int32),
            pltpu.VMEM((4, 4, 8, 16, 128), bf16),
            pltpu.VMEM((4, 16, 128), bf16),
            pltpu.VMEM((KL, 128), bf16),
            pltpu.VMEM((4, 4, 8, 16, 128), f32),
            pltpu.VMEM((32, KL), f32),
            pltpu.VMEM((KL // 8, 8, 128), f32),
            pltpu.VMEM((4, 4, 8, KL), f32),
            pltpu.VMEM((4, 4, 8, KL), f32),
            pltpu.VMEM((NE, 8, 8, 128), f32),
            pltpu.VMEM((NE, 8, 8, 128), f32),
            pltpu.VMEM((8, 128), f32),
            pltpu.VMEM((32, 128), jnp.int32),
            pltpu.VMEM((2, 32, 128), f32),
            pltpu.VMEM((128, KL), bf16),
            pltpu.VMEM((2, 4, 2, 64, 128), f32),
            dma((9,)), dma((2,)), dma((2,)), dma((2,)),
            dma((NE,)), dma((NE,)), dma((NE,)), dma((NE,)), dma((4,)), dma((4,)),
        ],
        compiler_params=pltpu.CompilerParams(
            collective_id=0, has_side_effects=True, vmem_limit_bytes=58_000_000
        ),
    )(
        positions,
        positions.reshape(1, 128),
        query_latent.transpose(1, 2, 0),
        key_latent.T,
        index_query.reshape(16, 8, 16, 128),
        index_weight.T,
        index_key,
    )
    return pl.pallas_call(
        results,
        out_shape=(
            jax.ShapeDtypeStruct((32, KL), f32),
            jax.ShapeDtypeStruct((32,), f32),
        ),
        in_specs=[vmem, vmem],
        out_specs=(vmem, vmem),
        compiler_params=pltpu.CompilerParams(vmem_limit_bytes=66_000_000),
    )(target, divergence)


def solution(mesh):
    finer = Mesh(
        mesh.devices.reshape(8, 4, 2, mesh.shape["head"]), ("z", "y", "c", "x")
    )
    return jax.shard_map(
        local,
        mesh=finer,
        in_specs=(
            P(None, "x", None),
            P(CTX, None),
            P(None, "x", None),
            P(None, "x"),
            P(CTX, None),
            P(),
        ),
        out_specs=(P("x", CTX), P("x")),
        check_vma=False,
    )
```

```python
import functools

import jax
import jax.numpy as jnp
from jax import lax
from jax.experimental import pallas as pl
from jax.experimental.pallas import tpu as pltpu
from jax.sharding import Mesh
from jax.sharding import PartitionSpec as P

H = 128
CTX = ("z", "y", "c")
NEG = -1e30
MESH = pl.DeviceIdType.MESH
f32 = jnp.float32
KL = 2048
QK = 576
PIECE = 256
NE = 5


def build_weights(q_ref, w_ref, t):
    group = (lax.broadcasted_iota(jnp.int32, (QK, 128), 1) // 8) % 4
    c = t // 4
    for j in range(2):
        i = (t % 4) * 2 + j
        out = None
        for g in range(4):
            r = pltpu.roll(q_ref[4 * i + g], lax.rem(8 * (g - c) + 128, 128), 1)
            out = r if out is None else jnp.where(group == g, r, out)
        w_ref[:, j * 128 : (j + 1) * 128] = out


def score_step(new_ref, old_ref, k_ref, w_ref, e_ref, top_ref, sum_ref, thr_ref, t, new=True,
               old=True, before=None):
    nt = t + 1
    biggest = [[None] * 8 for _ in range(2)]
    total = [None] * 2
    if new:
        th = thr_ref[nt // 4]
        w = w_ref[...]
    if old:
        tops = [jnp.broadcast_to(top_ref[pl.ds(2 * t + j, 1), :], (8, 128)) for j in range(2)]
    for p in range(KL // PIECE):
        if before is not None:
            before(p)
        rows = slice(p * PIECE, (p + 1) * PIECE)
        if new:
            r = lax.dot_general(
                k_ref[rows, :], w, (((1,), (0,)), ((), ())), preferred_element_type=f32
            )
            for k in range(PIECE // 8):
                at = p * PIECE + 8 * k
                m = th >= at
                for j in range(2):
                    v = jnp.where(m, r[8 * k : 8 * k + 8, j * 128 : (j + 1) * 128], NEG)
                    new_ref[at : at + 8, j * 128 : (j + 1) * 128] = v
                    a = k % 8
                    biggest[j][a] = v if biggest[j][a] is None else jnp.maximum(biggest[j][a], v)
        if old:
            for k in range(PIECE // 8):
                at = p * PIECE + 8 * k
                for j in range(2):
                    v = jnp.exp(old_ref[at : at + 8, j * 128 : (j + 1) * 128] - tops[j])
                    e_ref[t // 4, at // 8, (t % 4) * 2 + j] = v
                    total[j] = v if total[j] is None else total[j] + v
    for j in range(2):
        if new:
            m = jnp.max(functools.reduce(jnp.maximum, biggest[j]), axis=0, keepdims=True)
            top_ref[pl.ds(2 * nt + j, 1), :] = jnp.maximum(m, 0.5 * NEG)
        if old:
            sum_ref[pl.ds(2 * t + j, 1), :] = jnp.sum(total[j], axis=0, keepdims=True)


def lse_of(top, total):
    some = total > 0
    return jnp.where(some, top + jnp.log(jnp.where(some, total, 1.0)), NEG)


def merge_lse(v):
    m = jnp.max(v, axis=0)
    return m + jnp.log(jnp.sum(jnp.exp(v - m[None]), axis=0))


def as_row(column):
    n = column.shape[0]
    row = lax.broadcasted_iota(jnp.int32, (n, 128), 0)
    lane = lax.broadcasted_iota(jnp.int32, (n, 128), 1)
    return jnp.sum(jnp.where(row == lane, column, 0.0), axis=0, keepdims=True)


def kernel(
    pos_s, pos_v, q_hbm, k_hbm, iq_hbm, iw_hbm, ik_hbm,
    tgt_ref, div_ref,
    q_ref, kt_ref, k_ref, w0_ref, w1_ref, s0_ref, s1_ref, e_ref, top_ref, sum_ref, thr_ref,
    iq_ref, iw_ref, ik_ref, wc_ref, lg_ref, u_ref, part_ref, got_ref,
    ab_ref, bb_ref, l_ref, pc_ref, cm_ref, ikt_ref, f_ref, fin_ref,
    in_sem, ix_sem, ix_send, ix_recv, a_send, a_recv, b_send, b_recv, r_send, r_recv, f_send, f_recv,
):
    z, y, c0, x = (lax.axis_index(n) for n in ("z", "y", "c", "x"))
    me_a = y * 2 + c0
    base = ((z * 4 + y) * 2 + c0) * KL

    def x_peer(d):
        return {"z": z, "y": y, "c": c0, "x": lax.rem(x + d, 4)}

    def a_peer(d):
        p = lax.rem(me_a + d, 8)
        return {"z": z, "y": p // 2, "c": lax.rem(p, 2), "x": x}

    def b_peer(d):
        return {"z": lax.rem(z + d, 8), "y": y, "c": c0, "x": x}

    me_c = (z * 4 + y) * 2 + c0

    def c_peer(d):
        p = lax.rem(me_c + d, 64)
        return {"z": p // 8, "y": lax.rem(p // 2, 4), "c": lax.rem(p, 2), "x": x}

    k_in = [
        pltpu.make_async_copy(
            k_hbm.at[:, pl.ds(n * 512, 512)], kt_ref.at[:, pl.ds(n * 512, 512)], in_sem.at[n]
        )
        for n in range(4)
    ]
    q_in = [
        pltpu.make_async_copy(
            q_hbm.at[pl.ds(n * 8, 8)], q_ref.at[pl.ds(n * 8, 8)], in_sem.at[4 + n]
        )
        for n in range(4)
    ]
    ik_in = pltpu.make_async_copy(ik_hbm, ik_ref, in_sem.at[8])
    q_in[0].start()
    for cp in k_in:
        cp.start()
    own_iq = pltpu.make_async_copy(
        iq_hbm.at[pl.ds(x * 4, 4)], iq_ref.at[:, x], ix_sem.at[0]
    )
    own_iw = pltpu.make_async_copy(iw_hbm, iw_ref.at[x], ix_sem.at[1])
    own_iq.start()
    own_iw.start()

    barrier = pltpu.get_barrier_semaphore()
    for d in range(1, 4):
        pl.semaphore_signal(barrier, inc=1, device_id=x_peer(d), device_id_type=MESH)
    for d in range(1, 64):
        pl.semaphore_signal(barrier, inc=1, device_id=c_peer(d), device_id_type=MESH)

    group = (lax.broadcasted_iota(jnp.int32, (8, 128), 1) // 8) % 4
    sub = lax.broadcasted_iota(jnp.int32, (8, 128), 0)
    pos8 = jnp.broadcast_to(pos_v[...], (8, 128))
    for c in range(4):
        th = pos8
        for g in range(4):
            if g != c:
                th = jnp.where(group == g, pltpu.roll(pos8, (8 * (g - c)) % 128, 1), th)
        thr_ref[c] = th - base - sub
    for q in range(32):
        pc_ref[q : q + 1, :] = jnp.full((1, 128), pos_s[x * 32 + q] - base, jnp.int32)

    q_in[0].wait()
    build_weights(q_ref, w0_ref, 0)

    def key_block(p):
        if p % (512 // PIECE) == 0:
            k_in[p * PIECE // 512].wait()
        if p == 0:
            for cp in q_in[1:]:
                cp.start()
            ik_in.start()
        for n in range(PIECE // 128):
            at = p * PIECE + n * 128
            k_ref[at : at + 128, :] = kt_ref[:, at : at + 128].T

    score_step(
        s1_ref, s0_ref, k_ref, w0_ref, e_ref, top_ref, sum_ref, thr_ref, -1, old=False,
        before=key_block,
    )
    for cp in q_in[1:]:
        cp.wait()
    build_weights(q_ref, w1_ref, 1)

    pl.semaphore_wait(barrier, 66)
    own_iq.wait()
    own_iw.wait()

    def ix_copies(d):
        peer = x_peer(d)
        to = lax.rem(x + d, 4)
        return [
            pltpu.make_async_remote_copy(
                iq_hbm.at[pl.ds(to * 4, 4)], iq_ref.at[:, x],
                ix_send.at[0], ix_recv.at[0], device_id=peer, device_id_type=MESH,
            ),
            pltpu.make_async_remote_copy(
                iw_hbm, iw_ref.at[x],
                ix_send.at[1], ix_recv.at[1], device_id=peer, device_id_type=MESH,
            ),
        ]

    for d in range(1, 4):
        for cp in ix_copies(d):
            cp.start()

    def ix_all():
        return [
            pltpu.make_async_remote_copy(
                ref, ref, ix_send.at[k], ix_recv.at[k],
                device_id=x_peer(1), device_id_type=MESH,
            )
            for k, ref in enumerate((iq_ref.at[:, pl.ds(0, 3)], iw_ref.at[pl.ds(0, 3)]))
        ]

    def exchange_start(buf, me, e, value, send, recv, peer):
        buf[e, me] = value
        for d in range(1, 8):
            pltpu.make_async_remote_copy(
                buf.at[e, me], buf.at[e, me], send.at[e], recv.at[e],
                device_id=peer(d), device_id_type=MESH,
            ).start()

    def seven(buf, e, send, recv):
        return pltpu.make_async_remote_copy(
            buf.at[e, pl.ds(0, 7)], buf.at[e, pl.ds(0, 7)], send.at[e], recv.at[e],
            device_id=x_peer(1), device_id_type=MESH,
        )

    def a_start(e, value):
        exchange_start(ab_ref, me_a, e, value, a_send, a_recv, a_peer)

    def a_done(e):
        seven(ab_ref, e, a_send, a_recv).wait_recv()
        return ab_ref[e]

    def b_start(e, value):
        exchange_start(bb_ref, z, e, value, b_send, b_recv, b_peer)

    def b_done(e):
        seven(bb_ref, e, b_send, b_recv).wait_recv()
        return bb_ref[e]

    def stats_out(c):
        rows = pl.ds(pl.multiple_of(c * 8, 8), 8)
        a_start(c, lse_of(top_ref[rows, :], sum_ref[rows, :]))

    def middle(c):
        b_start(c, merge_lse(a_done(c)))

    def head_sum(c):
        lse = merge_lse(b_done(c))
        rows = pl.ds(pl.multiple_of(c * 8, 8), 8)
        l_ref[...] = jnp.exp(top_ref[rows, :] - lse) * (1.0 / H)
        coef = [jnp.broadcast_to(l_ref[i : i + 1, :], (8, 128)) for i in range(8)]

        for h in range(2):

            @pl.loop(h * 4, h * 4 + 4)
            def _(b):
                for k in range(32):
                    at = b * 32 + k
                    s = e_ref[c, at, 0] * coef[0]
                    for i in range(1, 8):
                        s = s + e_ref[c, at, i] * coef[i]
                    u_ref[at] = s

            for n in range(8):
                m = h * 8 + n
                v = u_ref[m * 16 : m * 16 + 16].reshape(128, 128).T
                for k in range(4):
                    r = [v[32 * k + 8 * g : 32 * k + 8 * g + 8, :] for g in range(4)]
                    part_ref[c, h, k, :, n * 128 : (n + 1) * 128] = (r[0] + r[1]) + (r[2] + r[3])
            for d in range(1, 4):
                to = lax.rem(x + d, 4)
                pltpu.make_async_remote_copy(
                    part_ref.at[c, h, to], got_ref.at[c, x, h],
                    r_send.at[c], r_recv.at[c], device_id=x_peer(d), device_id_type=MESH,
                ).start()

    def three(c):
        return pltpu.make_async_remote_copy(
            got_ref.at[c, pl.ds(0, 3)], got_ref.at[c, pl.ds(0, 3)],
            r_send.at[c], r_recv.at[c], device_id=x_peer(1), device_id_type=MESH,
        )

    def own_rows(c):
        three(c).wait_recv()
        for h in range(2):
            got_ref[c, x, h] = part_ref[c, h, x]
        rows = slice(8 * c, 8 * c + 8)
        cross = [None] * 4
        mass = [None] * 4
        for n in range(16):
            at = slice(n * 128, (n + 1) * 128)
            h, to = n // 8, slice(n % 8 * 128, n % 8 * 128 + 128)
            t = (got_ref[c, 0, h, :, to] + got_ref[c, 1, h, :, to]) + (
                got_ref[c, 2, h, :, to] + got_ref[c, 3, h, :, to]
            )
            tgt_ref[rows, at] = t
            positive = t > 0
            log = jnp.log(jnp.where(positive, t, 1.0))
            term = jnp.where(positive, t * log, 0.0) - t * lg_ref[rows, at]
            a = n % 4
            cross[a] = term if cross[a] is None else cross[a] + term
            mass[a] = t if mass[a] is None else mass[a] + t
        cross = (cross[0] + cross[1]) + (cross[2] + cross[3])
        mass = (mass[0] + mass[1]) + (mass[2] + mass[3])
        cm_ref[0, 8 * c : 8 * c + 8, :] = jnp.broadcast_to(
            jnp.sum(cross, axis=1, keepdims=True), (8, 128)
        )
        cm_ref[1, 8 * c : 8 * c + 8, :] = jnp.broadcast_to(
            jnp.sum(mass, axis=1, keepdims=True), (8, 128)
        )

    @pl.loop(0, 4)
    def _(c):
        @pl.loop(0, 2)
        def _(h):
            t = c * 4 + h * 2
            build_weights(q_ref, w0_ref, jnp.minimum(t + 2, 15))
            score_step(s0_ref, s1_ref, k_ref, w1_ref, e_ref, top_ref, sum_ref, thr_ref, t)

            @pl.when(t < 14)
            def _():
                build_weights(q_ref, w1_ref, jnp.minimum(t + 3, 15))
                score_step(s1_ref, s0_ref, k_ref, w0_ref, e_ref, top_ref, sum_ref, thr_ref, t + 1)

            @pl.when(t == 14)
            def _():
                score_step(
                    s1_ref, s0_ref, k_ref, w0_ref, e_ref, top_ref, sum_ref, thr_ref, t + 1,
                    new=False,
                )

        stats_out(c)

        @pl.when(c >= 1)
        def _():
            middle(c - 1)

    head_sum(0)
    head_sum(1)

    for cp in ix_all():
        cp.wait_recv()
    ik_in.wait()
    for n in range(KL // 128):
        ikt_ref[:, n * 128 : (n + 1) * 128] = ik_ref[n * 128 : (n + 1) * 128, :].T
    for k in range(4):
        w = pltpu.roll(iw_ref[k].astype(f32), lax.rem(128 - 32 * x, 128), 1)
        for q in range(32):
            wc_ref[q // 8, k, q % 8] = jnp.broadcast_to(w[:, q : q + 1], (16, 128))

    def logits_block(n, s):
        at = pl.ds(pl.multiple_of(n * 256, 256), 256)
        keys = ikt_ref[:, at]
        for b in range(4):
            r = lax.dot_general(
                iq_ref[b].reshape(512, 128), keys, (((1,), (0,)), ((), ())),
                preferred_element_type=f32,
            )
            for q in range(8):
                acc = [None, None]
                for k in range(4):
                    for h in range(2):
                        o = k * 128 + q * 16 + h * 8
                        w = wc_ref[b, k, q, h * 8 : h * 8 + 8, :]
                        for j in range(2):
                            v = w * jnp.maximum(r[o : o + 8, j * 128 : (j + 1) * 128], 0.0)
                            acc[j] = v if acc[j] is None else acc[j] + v
                for j in range(2):
                    f_ref[s, b, j, q * 8 : q * 8 + 8, :] = acc[j]
        for b in range(4):
            for j in range(2):
                v = f_ref[s, b, j, pl.ds(0, 8, stride=8), :]
                for i in range(1, 8):
                    v = v + f_ref[s, b, j, pl.ds(i, 8, stride=8), :]
                lg_ref[8 * b : 8 * b + 8, pl.ds(pl.multiple_of(n * 256 + j * 128, 128), 128)] = v

    @pl.loop(0, 2)
    def _(n):
        logits_block(n * 2, 0)
        logits_block(n * 2 + 1, 1)

    middle(3)

    @pl.loop(2, 4)
    def _(n):
        logits_block(n * 2, 0)
        logits_block(n * 2 + 1, 1)

    head_sum(2)

    cols = []
    lane = lax.broadcasted_iota(jnp.int32, (8, KL), 1)
    for c in range(4):
        rows = slice(8 * c, 8 * c + 8)
        ok = lane <= jnp.broadcast_to(pc_ref[rows, 0:1], (8, KL))
        v = jnp.where(ok, lg_ref[rows, :], NEG)
        top = jnp.max(v, axis=1, keepdims=True)
        total = jnp.sum(jnp.where(ok, jnp.exp(v - top), 0.0), axis=1, keepdims=True)
        cols.append(lse_of(top, total))
    a_start(4, jnp.broadcast_to(as_row(jnp.concatenate(cols, axis=0)), (8, 128)))

    own_rows(0)
    head_sum(3)
    middle(4)
    for c in range(1, 4):
        own_rows(c)
    spread = merge_lse(b_done(4))
    value = as_row(cm_ref[0]) + spread * as_row(cm_ref[1])
    fin_ref[me_c] = value[0:1]
    for d in sorted(range(1, 64), key=lambda d: abs(d - 32)):
        pltpu.make_async_remote_copy(
            fin_ref.at[me_c], fin_ref.at[me_c], f_send.at[0], f_recv.at[0],
            device_id=c_peer(d), device_id_type=MESH,
        ).start()
    others = pltpu.make_async_remote_copy(
        fin_ref.at[pl.ds(0, 63)], fin_ref.at[pl.ds(0, 63)], f_send.at[0], f_recv.at[0],
        device_id=x_peer(1), device_id_type=MESH,
    )
    others.wait_recv()
    div_ref[...] = jnp.broadcast_to(jnp.sum(fin_ref[...], axis=0), (8, 128))

    others.wait_send()
    for cp in ix_all():
        cp.wait_send()
    for e in range(NE):
        seven(ab_ref, e, a_send, a_recv).wait_send()
        seven(bb_ref, e, b_send, b_recv).wait_send()
    for c in range(4):
        three(c).wait_send()


def results(sum_ref, row_ref, tgt_ref, div_ref):
    tgt_ref[...] = sum_ref[...]
    div_ref[...] = row_ref[0, 0:32]


def local(query_latent, key_latent, index_query, index_weight, index_key, positions):
    vmem = pl.BlockSpec(memory_space=pltpu.VMEM)
    hbm = pl.BlockSpec(memory_space=pl.ANY)
    bf16 = jnp.bfloat16
    dma = pltpu.SemaphoreType.DMA
    target, divergence = pl.pallas_call(
        kernel,
        out_shape=(
            jax.ShapeDtypeStruct((32, KL), f32),
            jax.ShapeDtypeStruct((8, 128), f32),
        ),
        in_specs=[pl.BlockSpec(memory_space=pltpu.SMEM), vmem, hbm, hbm, hbm, hbm, hbm],
        out_specs=(vmem, vmem),
        scratch_shapes=[
            pltpu.VMEM((32, 576, 128), bf16),
            pltpu.VMEM((576, KL), bf16),
            pltpu.VMEM((KL, 576), bf16),
            pltpu.VMEM((QK, 256), bf16),
            pltpu.VMEM((QK, 256), bf16),
            pltpu.VMEM((KL, 256), f32),
            pltpu.VMEM((KL, 256), f32),
            pltpu.VMEM((4, KL // 8, 8, 8, 128), f32),
            pltpu.VMEM((32, 128), f32),
            pltpu.VMEM((32, 128), f32),
            pltpu.VMEM((4, 8, 128), jnp.int32),
            pltpu.VMEM((4, 4, 8, 16, 128), bf16),
            pltpu.VMEM((4, 16, 128), bf16),
            pltpu.VMEM((KL, 128), bf16),
            pltpu.VMEM((4, 4, 8, 16, 128), f32),
            pltpu.VMEM((32, KL), f32),
            pltpu.VMEM((KL // 8, 8, 128), f32),
            pltpu.VMEM((4, 2, 4, 8, KL // 2), f32),
            pltpu.VMEM((4, 4, 2, 8, KL // 2), f32),
            pltpu.VMEM((NE, 8, 8, 128), f32),
            pltpu.VMEM((NE, 8, 8, 128), f32),
            pltpu.VMEM((8, 128), f32),
            pltpu.VMEM((32, 128), jnp.int32),
            pltpu.VMEM((2, 32, 128), f32),
            pltpu.VMEM((128, KL), bf16),
            pltpu.VMEM((2, 4, 2, 64, 128), f32),
            pltpu.VMEM((64, 1, 128), f32),
            dma((9,)), dma((2,)), dma((2,)), dma((2,)),
            dma((NE,)), dma((NE,)), dma((NE,)), dma((NE,)), dma((4,)), dma((4,)), dma((1,)), dma((1,)),
        ],
        compiler_params=pltpu.CompilerParams(
            collective_id=0, has_side_effects=True, vmem_limit_bytes=58_000_000
        ),
    )(
        positions,
        positions.reshape(1, 128),
        query_latent.transpose(1, 2, 0),
        key_latent.T,
        index_query.reshape(16, 8, 16, 128),
        index_weight.T,
        index_key,
    )
    return pl.pallas_call(
        results,
        out_shape=(
            jax.ShapeDtypeStruct((32, KL), f32),
            jax.ShapeDtypeStruct((32,), f32),
        ),
        in_specs=[vmem, vmem],
        out_specs=(vmem, vmem),
        compiler_params=pltpu.CompilerParams(vmem_limit_bytes=66_000_000),
    )(target, divergence)


def solution(mesh):
    finer = Mesh(
        mesh.devices.reshape(8, 4, 2, mesh.shape["head"]), ("z", "y", "c", "x")
    )
    return jax.shard_map(
        local,
        mesh=finer,
        in_specs=(
            P(None, "x", None),
            P(CTX, None),
            P(None, "x", None),
            P(None, "x"),
            P(CTX, None),
            P(),
        ),
        out_specs=(P("x", CTX), P("x")),
        check_vma=False,
    )
```

```python
import functools

import jax
import jax.numpy as jnp
from jax import lax
from jax.experimental import pallas as pl
from jax.experimental.pallas import tpu as pltpu
from jax.sharding import Mesh
from jax.sharding import PartitionSpec as P

H = 128
CTX = ("z", "y", "c")
NEG = -1e30
MESH = pl.DeviceIdType.MESH
f32 = jnp.float32
KL = 2048
QK = 576
PIECE = 256
NE = 5


def build_weights(q_ref, w_ref, t):
    group = (lax.broadcasted_iota(jnp.int32, (QK, 128), 1) // 8) % 4
    c = t // 4
    for j in range(2):
        i = (t % 4) * 2 + j
        out = None
        for g in range(4):
            r = pltpu.roll(q_ref[4 * i + g], lax.rem(8 * (g - c) + 128, 128), 1)
            out = r if out is None else jnp.where(group == g, r, out)
        w_ref[:, j * 128 : (j + 1) * 128] = out


def score_step(new_ref, old_ref, k_ref, w_ref, e_ref, top_ref, sum_ref, thr_ref, t, new=True,
               old=True, before=None):
    nt = t + 1
    biggest = [[None] * 8 for _ in range(2)]
    total = [None] * 2
    if new:
        th = thr_ref[nt // 4]
        w = w_ref[...]
    if old:
        tops = [jnp.broadcast_to(top_ref[pl.ds(2 * t + j, 1), :], (8, 128)) for j in range(2)]
    for p in range(KL // PIECE):
        if before is not None:
            before(p)
        rows = slice(p * PIECE, (p + 1) * PIECE)
        if new:
            r = lax.dot_general(
                k_ref[rows, :], w, (((1,), (0,)), ((), ())), preferred_element_type=f32
            )
            for k in range(PIECE // 8):
                at = p * PIECE + 8 * k
                m = th >= at
                for j in range(2):
                    v = jnp.where(m, r[8 * k : 8 * k + 8, j * 128 : (j + 1) * 128], NEG)
                    new_ref[at : at + 8, j * 128 : (j + 1) * 128] = v
                    a = k % 8
                    biggest[j][a] = v if biggest[j][a] is None else jnp.maximum(biggest[j][a], v)
        if old:
            for k in range(PIECE // 8):
                at = p * PIECE + 8 * k
                for j in range(2):
                    v = jnp.exp(old_ref[at : at + 8, j * 128 : (j + 1) * 128] - tops[j])
                    e_ref[t // 4, at // 8, (t % 4) * 2 + j] = v
                    total[j] = v if total[j] is None else total[j] + v
    for j in range(2):
        if new:
            m = jnp.max(functools.reduce(jnp.maximum, biggest[j]), axis=0, keepdims=True)
            top_ref[pl.ds(2 * nt + j, 1), :] = jnp.maximum(m, 0.5 * NEG)
        if old:
            sum_ref[pl.ds(2 * t + j, 1), :] = jnp.sum(total[j], axis=0, keepdims=True)


def lse_of(top, total):
    some = total > 0
    return jnp.where(some, top + jnp.log(jnp.where(some, total, 1.0)), NEG)


def merge_lse(v):
    m = jnp.max(v, axis=0)
    return m + jnp.log(jnp.sum(jnp.exp(v - m[None]), axis=0))


def as_row(column):
    n = column.shape[0]
    row = lax.broadcasted_iota(jnp.int32, (n, 128), 0)
    lane = lax.broadcasted_iota(jnp.int32, (n, 128), 1)
    return jnp.sum(jnp.where(row == lane, column, 0.0), axis=0, keepdims=True)


def kernel(
    pos_s, pos_v, q_hbm, k_hbm, iq_hbm, iw_hbm, ik_hbm,
    tgt_ref, div_ref,
    q_ref, kt_ref, k_ref, w0_ref, w1_ref, s0_ref, s1_ref, e_ref, top_ref, sum_ref, thr_ref,
    iq_ref, iw_ref, ik_ref, wc_ref, lg_ref, u_ref, part_ref, got_ref,
    ab_ref, bb_ref, l_ref, pc_ref, cm_ref, ikt_ref, f_ref, fin_ref,
    in_sem, ix_sem, ix_send, ix_recv, a_send, a_recv, b_send, b_recv, r_send, r_recv, f_send, f_recv,
):
    z, y, c0, x = (lax.axis_index(n) for n in ("z", "y", "c", "x"))
    me_a = y * 2 + c0
    base = ((z * 4 + y) * 2 + c0) * KL

    def x_peer(d):
        return {"z": z, "y": y, "c": c0, "x": lax.rem(x + d, 4)}

    def a_peer(d):
        p = lax.rem(me_a + d, 8)
        return {"z": z, "y": p // 2, "c": lax.rem(p, 2), "x": x}

    def b_peer(d):
        return {"z": lax.rem(z + d, 8), "y": y, "c": c0, "x": x}

    me_c = (z * 4 + y) * 2 + c0

    def c_peer(d):
        p = lax.rem(me_c + d, 64)
        return {"z": p // 8, "y": lax.rem(p // 2, 4), "c": lax.rem(p, 2), "x": x}

    k_in = [
        pltpu.make_async_copy(
            k_hbm.at[:, pl.ds(n * 512, 512)], kt_ref.at[:, pl.ds(n * 512, 512)], in_sem.at[n]
        )
        for n in range(4)
    ]
    q_in = [
        pltpu.make_async_copy(
            q_hbm.at[pl.ds(n * 8, 8)], q_ref.at[pl.ds(n * 8, 8)], in_sem.at[4 + n]
        )
        for n in range(4)
    ]
    ik_in = pltpu.make_async_copy(ik_hbm, ik_ref, in_sem.at[8])
    q_in[0].start()
    for cp in k_in:
        cp.start()
    own_iq = pltpu.make_async_copy(
        iq_hbm.at[pl.ds(x * 4, 4)], iq_ref.at[:, x], ix_sem.at[0]
    )
    own_iw = pltpu.make_async_copy(iw_hbm, iw_ref.at[x], ix_sem.at[1])
    own_iq.start()
    own_iw.start()

    barrier = pltpu.get_barrier_semaphore()
    for d in range(1, 4):
        pl.semaphore_signal(barrier, inc=1, device_id=x_peer(d), device_id_type=MESH)
    for d in range(1, 64):
        pl.semaphore_signal(barrier, inc=1, device_id=c_peer(d), device_id_type=MESH)

    group = (lax.broadcasted_iota(jnp.int32, (8, 128), 1) // 8) % 4
    sub = lax.broadcasted_iota(jnp.int32, (8, 128), 0)
    pos8 = jnp.broadcast_to(pos_v[...], (8, 128))
    for c in range(4):
        th = pos8
        for g in range(4):
            if g != c:
                th = jnp.where(group == g, pltpu.roll(pos8, (8 * (g - c)) % 128, 1), th)
        thr_ref[c] = th - base - sub
    for q in range(32):
        pc_ref[q : q + 1, :] = jnp.full((1, 128), pos_s[x * 32 + q] - base, jnp.int32)

    q_in[0].wait()
    build_weights(q_ref, w0_ref, 0)

    def key_block(p):
        if p % (512 // PIECE) == 0:
            k_in[p * PIECE // 512].wait()
        if p == 0:
            for cp in q_in[1:]:
                cp.start()
            ik_in.start()
        for n in range(PIECE // 128):
            at = p * PIECE + n * 128
            k_ref[at : at + 128, :] = kt_ref[:, at : at + 128].T

    score_step(
        s1_ref, s0_ref, k_ref, w0_ref, e_ref, top_ref, sum_ref, thr_ref, -1, old=False,
        before=key_block,
    )
    for cp in q_in[1:]:
        cp.wait()
    build_weights(q_ref, w1_ref, 1)

    pl.semaphore_wait(barrier, 66)
    own_iq.wait()
    own_iw.wait()

    def ix_copies(d):
        peer = x_peer(d)
        to = lax.rem(x + d, 4)
        return [
            pltpu.make_async_remote_copy(
                iq_hbm.at[pl.ds(to * 4, 4)], iq_ref.at[:, x],
                ix_send.at[0], ix_recv.at[0], device_id=peer, device_id_type=MESH,
            ),
            pltpu.make_async_remote_copy(
                iw_hbm, iw_ref.at[x],
                ix_send.at[1], ix_recv.at[1], device_id=peer, device_id_type=MESH,
            ),
        ]

    for d in range(1, 4):
        for cp in ix_copies(d):
            cp.start()

    def ix_all():
        return [
            pltpu.make_async_remote_copy(
                ref, ref, ix_send.at[k], ix_recv.at[k],
                device_id=x_peer(1), device_id_type=MESH,
            )
            for k, ref in enumerate((iq_ref.at[:, pl.ds(0, 3)], iw_ref.at[pl.ds(0, 3)]))
        ]

    def exchange_start(buf, me, e, value, send, recv, peer):
        buf[e, me] = value
        for d in range(1, 8):
            pltpu.make_async_remote_copy(
                buf.at[e, me], buf.at[e, me], send.at[e], recv.at[e],
                device_id=peer(d), device_id_type=MESH,
            ).start()

    def seven(buf, e, send, recv):
        return pltpu.make_async_remote_copy(
            buf.at[e, pl.ds(0, 7)], buf.at[e, pl.ds(0, 7)], send.at[e], recv.at[e],
            device_id=x_peer(1), device_id_type=MESH,
        )

    def a_start(e, value):
        exchange_start(ab_ref, me_a, e, value, a_send, a_recv, a_peer)

    def a_done(e):
        seven(ab_ref, e, a_send, a_recv).wait_recv()
        return ab_ref[e]

    def b_start(e, value):
        exchange_start(bb_ref, z, e, value, b_send, b_recv, b_peer)

    def b_done(e):
        seven(bb_ref, e, b_send, b_recv).wait_recv()
        return bb_ref[e]

    def stats_out(c):
        rows = pl.ds(pl.multiple_of(c * 8, 8), 8)
        a_start(c, lse_of(top_ref[rows, :], sum_ref[rows, :]))

    def middle(c):
        b_start(c, merge_lse(a_done(c)))

    def head_sum(c):
        lse = merge_lse(b_done(c))
        rows = pl.ds(pl.multiple_of(c * 8, 8), 8)
        l_ref[...] = jnp.exp(top_ref[rows, :] - lse) * (1.0 / H)
        coef = [jnp.broadcast_to(l_ref[i : i + 1, :], (8, 128)) for i in range(8)]

        for h in range(2):

            @pl.loop(h * 4, h * 4 + 4)
            def _(b):
                for k in range(32):
                    at = b * 32 + k
                    s = e_ref[c, at, 0] * coef[0]
                    for i in range(1, 8):
                        s = s + e_ref[c, at, i] * coef[i]
                    u_ref[at] = s

            for n in range(8):
                m = h * 8 + n
                v = u_ref[m * 16 : m * 16 + 16].reshape(128, 128).T
                for k in range(4):
                    r = [v[32 * k + 8 * g : 32 * k + 8 * g + 8, :] for g in range(4)]
                    part_ref[c, h, k, :, n * 128 : (n + 1) * 128] = (r[0] + r[1]) + (r[2] + r[3])
            for d in range(1, 4):
                to = lax.rem(x + d, 4)
                pltpu.make_async_remote_copy(
                    part_ref.at[c, h, to], got_ref.at[c, x, h],
                    r_send.at[c], r_recv.at[c], device_id=x_peer(d), device_id_type=MESH,
                ).start()

    def three(c):
        return pltpu.make_async_remote_copy(
            got_ref.at[c, pl.ds(0, 3)], got_ref.at[c, pl.ds(0, 3)],
            r_send.at[c], r_recv.at[c], device_id=x_peer(1), device_id_type=MESH,
        )

    def own_rows(c):
        three(c).wait_recv()
        for h in range(2):
            got_ref[c, x, h] = part_ref[c, h, x]
        rows = slice(8 * c, 8 * c + 8)
        cross = [None] * 4
        mass = [None] * 4
        for n in range(16):
            at = slice(n * 128, (n + 1) * 128)
            h, to = n // 8, slice(n % 8 * 128, n % 8 * 128 + 128)
            t = (got_ref[c, 0, h, :, to] + got_ref[c, 1, h, :, to]) + (
                got_ref[c, 2, h, :, to] + got_ref[c, 3, h, :, to]
            )
            tgt_ref[rows, at] = t
            positive = t > 0
            log = jnp.log(jnp.where(positive, t, 1.0))
            term = jnp.where(positive, t * log, 0.0) - t * lg_ref[rows, at]
            a = n % 4
            cross[a] = term if cross[a] is None else cross[a] + term
            mass[a] = t if mass[a] is None else mass[a] + t
        cross = (cross[0] + cross[1]) + (cross[2] + cross[3])
        mass = (mass[0] + mass[1]) + (mass[2] + mass[3])
        cm_ref[0, 8 * c : 8 * c + 8, :] = jnp.broadcast_to(
            jnp.sum(cross, axis=1, keepdims=True), (8, 128)
        )
        cm_ref[1, 8 * c : 8 * c + 8, :] = jnp.broadcast_to(
            jnp.sum(mass, axis=1, keepdims=True), (8, 128)
        )

    @pl.loop(0, 4)
    def _(c):
        @pl.loop(0, 2)
        def _(h):
            t = c * 4 + h * 2
            build_weights(q_ref, w0_ref, jnp.minimum(t + 2, 15))
            score_step(s0_ref, s1_ref, k_ref, w1_ref, e_ref, top_ref, sum_ref, thr_ref, t)

            @pl.when(t < 14)
            def _():
                build_weights(q_ref, w1_ref, jnp.minimum(t + 3, 15))
                score_step(s1_ref, s0_ref, k_ref, w0_ref, e_ref, top_ref, sum_ref, thr_ref, t + 1)

            @pl.when(t == 14)
            def _():
                score_step(
                    s1_ref, s0_ref, k_ref, w0_ref, e_ref, top_ref, sum_ref, thr_ref, t + 1,
                    new=False,
                )

        stats_out(c)

        @pl.when(c >= 1)
        def _():
            middle(c - 1)

    head_sum(0)
    head_sum(1)

    for cp in ix_all():
        cp.wait_recv()
    ik_in.wait()
    for n in range(KL // 128):
        ikt_ref[:, n * 128 : (n + 1) * 128] = ik_ref[n * 128 : (n + 1) * 128, :].T
    for k in range(4):
        w = pltpu.roll(iw_ref[k].astype(f32), lax.rem(128 - 32 * x, 128), 1)
        for q in range(32):
            wc_ref[q // 8, k, q % 8] = jnp.broadcast_to(w[:, q : q + 1], (16, 128))

    def logits_block(n, s):
        at = pl.ds(n * 256 if isinstance(n, int) else pl.multiple_of(n * 256, 256), 256)
        keys = ikt_ref[:, at]
        for b in range(4):
            r = lax.dot_general(
                iq_ref[b].reshape(512, 128), keys, (((1,), (0,)), ((), ())),
                preferred_element_type=f32,
            )
            for q in range(8):
                acc = [None, None]
                for k in range(4):
                    for h in range(2):
                        o = k * 128 + q * 16 + h * 8
                        w = wc_ref[b, k, q, h * 8 : h * 8 + 8, :]
                        for j in range(2):
                            v = w * jnp.maximum(r[o : o + 8, j * 128 : (j + 1) * 128], 0.0)
                            acc[j] = v if acc[j] is None else acc[j] + v
                for j in range(2):
                    f_ref[s, b, j, q * 8 : q * 8 + 8, :] = acc[j]
        for b in range(4):
            for j in range(2):
                v = f_ref[s, b, j, pl.ds(0, 8, stride=8), :]
                for i in range(1, 8):
                    v = v + f_ref[s, b, j, pl.ds(i, 8, stride=8), :]
                lg_ref[8 * b : 8 * b + 8, pl.ds(
                    n * 256 + j * 128 if isinstance(n, int)
                    else pl.multiple_of(n * 256 + j * 128, 128), 128,
                )] = v

    logits_block(0, 0)
    logits_block(1, 1)

    middle(3)

    @pl.loop(1, 4)
    def _(n):
        logits_block(n * 2, 0)
        logits_block(n * 2 + 1, 1)

    head_sum(2)

    cols = []
    lane = lax.broadcasted_iota(jnp.int32, (8, KL), 1)
    for c in range(4):
        rows = slice(8 * c, 8 * c + 8)
        ok = lane <= jnp.broadcast_to(pc_ref[rows, 0:1], (8, KL))
        v = jnp.where(ok, lg_ref[rows, :], NEG)
        top = jnp.max(v, axis=1, keepdims=True)
        total = jnp.sum(jnp.where(ok, jnp.exp(v - top), 0.0), axis=1, keepdims=True)
        cols.append(lse_of(top, total))
    a_start(4, jnp.broadcast_to(as_row(jnp.concatenate(cols, axis=0)), (8, 128)))

    own_rows(0)
    head_sum(3)
    middle(4)
    for c in range(1, 4):
        own_rows(c)
    spread = merge_lse(b_done(4))
    value = as_row(cm_ref[0]) + spread * as_row(cm_ref[1])
    fin_ref[me_c] = value[0:1]
    for d in sorted(range(1, 64), key=lambda d: abs(d - 32)):
        pltpu.make_async_remote_copy(
            fin_ref.at[me_c], fin_ref.at[me_c], f_send.at[0], f_recv.at[0],
            device_id=c_peer(d), device_id_type=MESH,
        ).start()
    others = pltpu.make_async_remote_copy(
        fin_ref.at[pl.ds(0, 63)], fin_ref.at[pl.ds(0, 63)], f_send.at[0], f_recv.at[0],
        device_id=x_peer(1), device_id_type=MESH,
    )
    for cp in ix_all():
        cp.wait_send()
    for e in range(NE):
        seven(ab_ref, e, a_send, a_recv).wait_send()
        seven(bb_ref, e, b_send, b_recv).wait_send()
    for c in range(4):
        three(c).wait_send()
    others.wait_recv()
    div_ref[...] = jnp.broadcast_to(jnp.sum(fin_ref[...], axis=0), (8, 128))
    others.wait_send()


def results(sum_ref, row_ref, tgt_ref, div_ref):
    tgt_ref[...] = sum_ref[...]
    div_ref[...] = row_ref[0, 0:32]


def local(query_latent, key_latent, index_query, index_weight, index_key, positions):
    vmem = pl.BlockSpec(memory_space=pltpu.VMEM)
    hbm = pl.BlockSpec(memory_space=pl.ANY)
    bf16 = jnp.bfloat16
    dma = pltpu.SemaphoreType.DMA
    target, divergence = pl.pallas_call(
        kernel,
        out_shape=(
            jax.ShapeDtypeStruct((32, KL), f32),
            jax.ShapeDtypeStruct((8, 128), f32),
        ),
        in_specs=[pl.BlockSpec(memory_space=pltpu.SMEM), vmem, hbm, hbm, hbm, hbm, hbm],
        out_specs=(vmem, vmem),
        scratch_shapes=[
            pltpu.VMEM((32, 576, 128), bf16),
            pltpu.VMEM((576, KL), bf16),
            pltpu.VMEM((KL, 576), bf16),
            pltpu.VMEM((QK, 256), bf16),
            pltpu.VMEM((QK, 256), bf16),
            pltpu.VMEM((KL, 256), f32),
            pltpu.VMEM((KL, 256), f32),
            pltpu.VMEM((4, KL // 8, 8, 8, 128), f32),
            pltpu.VMEM((32, 128), f32),
            pltpu.VMEM((32, 128), f32),
            pltpu.VMEM((4, 8, 128), jnp.int32),
            pltpu.VMEM((4, 4, 8, 16, 128), bf16),
            pltpu.VMEM((4, 16, 128), bf16),
            pltpu.VMEM((KL, 128), bf16),
            pltpu.VMEM((4, 4, 8, 16, 128), f32),
            pltpu.VMEM((32, KL), f32),
            pltpu.VMEM((KL // 8, 8, 128), f32),
            pltpu.VMEM((4, 2, 4, 8, KL // 2), f32),
            pltpu.VMEM((4, 4, 2, 8, KL // 2), f32),
            pltpu.VMEM((NE, 8, 8, 128), f32),
            pltpu.VMEM((NE, 8, 8, 128), f32),
            pltpu.VMEM((8, 128), f32),
            pltpu.VMEM((32, 128), jnp.int32),
            pltpu.VMEM((2, 32, 128), f32),
            pltpu.VMEM((128, KL), bf16),
            pltpu.VMEM((2, 4, 2, 64, 128), f32),
            pltpu.VMEM((64, 1, 128), f32),
            dma((9,)), dma((2,)), dma((2,)), dma((2,)),
            dma((NE,)), dma((NE,)), dma((NE,)), dma((NE,)), dma((4,)), dma((4,)), dma((1,)), dma((1,)),
        ],
        compiler_params=pltpu.CompilerParams(
            collective_id=0, has_side_effects=True, vmem_limit_bytes=58_000_000
        ),
    )(
        positions,
        positions.reshape(1, 128),
        query_latent.transpose(1, 2, 0),
        key_latent.T,
        index_query.reshape(16, 8, 16, 128),
        index_weight.T,
        index_key,
    )
    return pl.pallas_call(
        results,
        out_shape=(
            jax.ShapeDtypeStruct((32, KL), f32),
            jax.ShapeDtypeStruct((32,), f32),
        ),
        in_specs=[vmem, vmem],
        out_specs=(vmem, vmem),
        compiler_params=pltpu.CompilerParams(vmem_limit_bytes=66_000_000),
    )(target, divergence)


def solution(mesh):
    finer = Mesh(
        mesh.devices.reshape(8, 4, 2, mesh.shape["head"]), ("z", "y", "c", "x")
    )
    return jax.shard_map(
        local,
        mesh=finer,
        in_specs=(
            P(None, "x", None),
            P(CTX, None),
            P(None, "x", None),
            P(None, "x"),
            P(CTX, None),
            P(),
        ),
        out_specs=(P("x", CTX), P("x")),
        check_vma=False,
    )
```
